32 devices in a mesh: pair: 1 (over z), tp: 4 (over y), side: 8 (over x, core).
Axes of the slice: x: 4, y: 4, z: 1, core: 2. Of those that a mesh axis runs over, the one named last changes fastest.
The devices are a block of a 4x4x8 slice.
Arguments:
- prompt_x: bfloat16 [1024, 4096], P(('pair', 'side'))
- s_len: int32 [8], P(('pair', 'side'))
- w_qkv_pre: bfloat16 [1, 4096, 3, 32, 128], P(None, None, None, 'tp')
- w_out_pre: bfloat16 [1, 32, 128, 4096], P(None, 'tp')
- w_gu_pre: bfloat16 [1, 2, 11008, 4096], P(None, None, 'tp')
- w_down_pre: bfloat16 [1, 11008, 4096], P(None, 'tp')
- gain_pre: float32 [1, 2, 4096], replicated
- dec_tokens: bfloat16 [64, 4096], P(('pair', 'side'))
- k_cache: bfloat16 [1, 64, 256, 8, 4, 128], P(None, ('pair', 'side'), None, None, 'tp')
- v_cache: bfloat16 [1, 64, 256, 8, 4, 128], P(None, ('pair', 'side'), None, None, 'tp')
- c_len: int32 [64], P(('pair', 'side'))
- w_qkv_dec: bfloat16 [1, 4096, 3, 8, 4, 128], P(None, None, None, None, 'tp')
- w_out_dec: bfloat16 [1, 8, 4, 128, 4096], P(None, None, 'tp')
- w_gu_dec: bfloat16 [1, 2, 11008, 4096], P(None, None, 'tp')
- w_down_dec: bfloat16 [1, 11008, 4096], P(None, 'tp')
- gain_dec: float32 [1, 2, 4096], replicated
Outputs:
- output 1: bfloat16 [1024, 4096], P(('pair', 'side'))
- output 2: bfloat16 [64, 4096], P(('pair', 'side'))
- output 3: bfloat16 [1, 1024, 8, 4, 128], P(None, ('pair', 'side'), None, 'tp')
- output 4: bfloat16 [1, 1024, 8, 4, 128], P(None, ('pair', 'side'), None, 'tp')
- output 5: bfloat16 [1, 64, 256, 8, 4, 128], P(None, ('pair', 'side'), None, None, 'tp')
- output 6: bfloat16 [1, 64, 256, 8, 4, 128], P(None, ('pair', 'side'), None, None, 'tp')
All inputs are finite; a program needn't handle non-finite values.
Results may differ from the reference program's by a relative error of at most 0.0125934.
Values are sent between devices in bfloat16 or wider.
A program may use at most 768 MiB of HBM per device.

```python
import jax
import jax.numpy as jnp
from jax import lax

D = 4096
HEADS = 32
HEAD = 128
FF = 11008
LAYERS = 1
PROMPT = 128
BATCH = 8
CACHE = 256
TP_SIZE = 4
SIDES = 8

EPSILON = 1e-6
THETA = 10000.0
QK_GAIN = 1.5
OUT_GAIN = 2.0
MASKED = -1e30


def draw_int_inputs(len_key, cache_key):
    low_prompt = PROMPT // 2
    len_keys = jax.random.split(len_key, 2)
    s_len = jax.random.randint(len_keys[0], (SIDES,), low_prompt, PROMPT + 1, dtype=jnp.int32)
    slot_top = jax.random.randint(len_keys[1], (), 0, SIDES, dtype=jnp.int32)
    s_len = s_len.at[slot_top].set(PROMPT).at[(slot_top + 1) % SIDES].set(low_prompt)
    low_cache = CACHE // 4
    row_total = SIDES * BATCH
    cache_keys = jax.random.split(cache_key, 2)
    c_len = jax.random.randint(cache_keys[0], (row_total,), low_cache, CACHE, dtype=jnp.int32)
    row_top = jax.random.randint(cache_keys[1], (), 0, row_total, dtype=jnp.int32)
    c_len = c_len.at[row_top].set(CACHE - 1).at[(row_top + 1) % row_total].set(low_cache)
    return s_len, c_len


def draw_weights(weight_key):
    weight_keys = jax.random.split(weight_key, 5)
    qkv_scale = jnp.array([QK_GAIN, QK_GAIN, 1.0], jnp.float32)[:, None, None] * D ** -0.5
    w_qkv = (jax.random.normal(weight_keys[0], (LAYERS, D, 3, HEADS, HEAD), jnp.float32) * qkv_scale).astype(jnp.bfloat16)
    w_out = (jax.random.normal(weight_keys[1], (LAYERS, HEADS, HEAD, D), jnp.float32) * (OUT_GAIN * (HEADS * HEAD) ** -0.5)).astype(jnp.bfloat16)
    w_gu = (jax.random.normal(weight_keys[2], (LAYERS, 2, FF, D), jnp.float32) * D ** -0.5).astype(jnp.bfloat16)
    w_down = (jax.random.normal(weight_keys[3], (LAYERS, FF, D), jnp.float32) * FF ** -0.5).astype(jnp.bfloat16)
    gains = jax.random.uniform(weight_keys[4], (LAYERS, 2, D), jnp.float32, 0.5, 1.5)
    return w_qkv, w_out, w_gu, w_down, gains


def setup_inputs(seed: int = 0, part: int = 0) -> dict:
    shared_keys = jax.random.split(jax.random.key(seed + 1), 2)
    part_keys = jax.random.split(jax.random.fold_in(jax.random.key(seed), part), 6)
    heads_tp = HEADS // TP_SIZE
    w_qkv_pre, w_out_pre, w_gu_pre, w_down_pre, gain_pre = draw_weights(shared_keys[0])
    w_qkv_dec, w_out_dec, w_gu_dec, w_down_dec, gain_dec = draw_weights(shared_keys[1])
    s_len, c_len = draw_int_inputs(part_keys[0], part_keys[1])
    prompt_x = jax.random.normal(part_keys[2], (SIDES * PROMPT, D), jnp.float32).astype(jnp.bfloat16)
    dec_tokens = jax.random.normal(part_keys[3], (SIDES * BATCH, D), jnp.float32).astype(jnp.bfloat16)
    cache_shape = (LAYERS, SIDES * BATCH, CACHE, heads_tp, TP_SIZE, HEAD)
    k_cache = (jax.random.normal(part_keys[4], cache_shape, jnp.float32) * QK_GAIN).astype(jnp.bfloat16)
    v_cache = jax.random.normal(part_keys[5], cache_shape, jnp.float32).astype(jnp.bfloat16)
    return {'prompt_x': prompt_x, 's_len': s_len, 'w_qkv_pre': w_qkv_pre, 'w_out_pre': w_out_pre, 'w_gu_pre': w_gu_pre, 'w_down_pre': w_down_pre, 'gain_pre': gain_pre, 'dec_tokens': dec_tokens, 'k_cache': k_cache, 'v_cache': v_cache, 'c_len': c_len, 'w_qkv_dec': w_qkv_dec.reshape(LAYERS, D, 3, heads_tp, TP_SIZE, HEAD), 'w_out_dec': w_out_dec.reshape(LAYERS, heads_tp, TP_SIZE, HEAD, D), 'w_gu_dec': w_gu_dec, 'w_down_dec': w_down_dec, 'gain_dec': gain_dec}


def rms_norm(hidden, gain_vec):
    hid_f32 = hidden.astype(jnp.float32)
    inv_rms = lax.rsqrt(jnp.mean(hid_f32 * hid_f32, axis=-1, keepdims=True) + EPSILON)
    return (hid_f32 * inv_rms * gain_vec).astype(jnp.bfloat16)


def add_residual(hidden, update):
    return (hidden.astype(jnp.float32) + update.astype(jnp.float32)).astype(jnp.bfloat16)


def rope_tables(positions):
    half_dim = HEAD // 2
    inv_freq = THETA ** (-jnp.arange(half_dim, dtype=jnp.float32) * 2.0 / HEAD)
    angles = positions.astype(jnp.float32)[:, None] * inv_freq[None, :]
    return jnp.cos(angles), jnp.sin(angles)


def apply_rope(values_in, cos_tab, sin_tab):
    half_dim = values_in.shape[-1] // 2
    lower_half = values_in[..., :half_dim]
    upper_half = values_in[..., half_dim:]
    cos_b = cos_tab[:, None, :]
    sin_b = sin_tab[:, None, :]
    return jnp.concatenate([lower_half * cos_b - upper_half * sin_b, upper_half * cos_b + lower_half * sin_b], axis=-1)


def mlp_block(hidden, gain_vec, w_gu, w_down):
    normed = rms_norm(hidden, gain_vec)
    gate_up = jnp.einsum('sd,kfd->skf', normed.astype(jnp.float32), w_gu.astype(jnp.float32))
    gate_val = gate_up[:, 0].astype(jnp.bfloat16).astype(jnp.float32)
    up_val = gate_up[:, 1].astype(jnp.bfloat16).astype(jnp.float32)
    activated = (jax.nn.silu(gate_val) * up_val).astype(jnp.bfloat16)
    down_out = jnp.dot(activated, w_down, preferred_element_type=jnp.float32).astype(jnp.bfloat16)
    return add_residual(hidden, down_out)


def prefill_one(x_inst, s_valid, w_qkv, w_out, w_gu, w_down, gains):
    positions = jnp.arange(PROMPT)
    cos_tab, sin_tab = rope_tables(positions)
    allowed = (positions[None, :] <= positions[:, None]) & (positions[None, :] < s_valid)

    def head_attention(head_in):
        q_head, k_head, v_head = head_in
        scores = jnp.einsum('qe,ke->qk', q_head.astype(jnp.float32), k_head.astype(jnp.float32)) * HEAD ** -0.5
        scores = jnp.where(allowed, scores, MASKED)
        prob_bf = jax.nn.softmax(scores, axis=-1).astype(jnp.bfloat16)
        return jnp.einsum('qk,ke->qe', prob_bf.astype(jnp.float32), v_head.astype(jnp.float32)).astype(jnp.bfloat16)

    def layer_step(hidden, layer_in):
        wqkv_l, wout_l, wgu_l, wdown_l, gain_l = layer_in
        normed = rms_norm(hidden, gain_l[0])
        qkv_out = jnp.einsum('sd,dkhe->skhe', normed.astype(jnp.float32), wqkv_l.astype(jnp.float32))
        queries = apply_rope(qkv_out[:, 0], cos_tab, sin_tab).astype(jnp.bfloat16)
        keys_new = apply_rope(qkv_out[:, 1], cos_tab, sin_tab).astype(jnp.bfloat16)
        values_new = qkv_out[:, 2].astype(jnp.bfloat16)
        context = lax.map(head_attention, (queries.transpose(1, 0, 2), keys_new.transpose(1, 0, 2), values_new.transpose(1, 0, 2)))
        attn_out = jnp.einsum('hse,hed->sd', context.astype(jnp.float32), wout_l.astype(jnp.float32)).astype(jnp.bfloat16)
        hidden = add_residual(hidden, attn_out)
        hidden = mlp_block(hidden, gain_l[1], wgu_l, wdown_l)
        return hidden, (keys_new, values_new)

    return lax.scan(layer_step, x_inst, (w_qkv, w_out, w_gu, w_down, gains))


def decode_rows(tokens, k_cache, v_cache, c_len, w_qkv, w_out, w_gu, w_down, gains):
    row_total = tokens.shape[0]
    cos_tab, sin_tab = rope_tables(c_len)
    cache_pos = jnp.arange(CACHE)
    k_flat = k_cache.reshape(LAYERS, row_total, CACHE, HEADS, HEAD)
    v_flat = v_cache.reshape(LAYERS, row_total, CACHE, HEADS, HEAD)
    wqkv_flat = w_qkv.reshape(LAYERS, D, 3, HEADS, HEAD)
    wout_flat = w_out.reshape(LAYERS, HEADS, HEAD, D)
    write_at = (cache_pos[None, :] == c_len[:, None])[:, :, None, None]

    def row_attention(row_in):
        q_row, k_row, v_row, kc_row, vc_row, len_row = row_in
        cache_scores = jnp.einsum('he,the->ht', q_row.astype(jnp.float32), kc_row.astype(jnp.float32)) * HEAD ** -0.5
        cache_scores = jnp.where(cache_pos[None, :] < len_row, cache_scores, MASKED)
        self_score = jnp.sum(q_row.astype(jnp.float32) * k_row.astype(jnp.float32), axis=-1) * HEAD ** -0.5
        joint_scores = jnp.concatenate([cache_scores, self_score[:, None]], axis=1)
        prob_bf = jax.nn.softmax(joint_scores, axis=-1).astype(jnp.bfloat16).astype(jnp.float32)
        context = jnp.einsum('ht,the->he', prob_bf[:, :CACHE], vc_row.astype(jnp.float32)) + prob_bf[:, CACHE:] * v_row.astype(jnp.float32)
        return context.astype(jnp.bfloat16)

    def layer_step(hidden, layer_in):
        wqkv_l, wout_l, wgu_l, wdown_l, gain_l, kc_l, vc_l = layer_in
        normed = rms_norm(hidden, gain_l[0])
        qkv_out = jnp.einsum('bd,dkhe->bkhe', normed.astype(jnp.float32), wqkv_l.astype(jnp.float32))
        queries = apply_rope(qkv_out[:, 0], cos_tab, sin_tab).astype(jnp.bfloat16)
        k_tok = apply_rope(qkv_out[:, 1], cos_tab, sin_tab).astype(jnp.bfloat16)
        v_tok = qkv_out[:, 2].astype(jnp.bfloat16)
        context = lax.map(row_attention, (queries, k_tok, v_tok, kc_l, vc_l, c_len))
        attn_out = jnp.einsum('bhe,hed->bd', context.astype(jnp.float32), wout_l.astype(jnp.float32)).astype(jnp.bfloat16)
        hidden = add_residual(hidden, attn_out)
        hidden = mlp_block(hidden, gain_l[1], wgu_l, wdown_l)
        kc_next = jnp.where(write_at, k_tok[:, None], kc_l)
        vc_next = jnp.where(write_at, v_tok[:, None], vc_l)
        return hidden, (kc_next, vc_next)

    final_tokens, (kc_all, vc_all) = lax.scan(layer_step, tokens, (wqkv_flat, wout_flat, w_gu, w_down, gains, k_flat, v_flat))
    return final_tokens, kc_all.reshape(k_cache.shape), vc_all.reshape(v_cache.shape)


def reference(prompt_x, s_len, w_qkv_pre, w_out_pre, w_gu_pre, w_down_pre, gain_pre, dec_tokens, k_cache, v_cache, c_len, w_qkv_dec, w_out_dec, w_gu_dec, w_down_dec, gain_dec):
    prompts = prompt_x.reshape(SIDES, PROMPT, D)

    def run_instance(inst_in):
        x_inst, s_valid = inst_in
        final_hidden, (k_all, v_all) = prefill_one(x_inst, s_valid, w_qkv_pre, w_out_pre, w_gu_pre, w_down_pre, gain_pre)
        return final_hidden, k_all, v_all

    final_hidden, k_all, v_all = lax.map(run_instance, (prompts, s_len))
    half_sides = SIDES // 2
    prompt_shape = (LAYERS, SIDES * PROMPT, HEADS // TP_SIZE, TP_SIZE, HEAD)
    k_prompt = jnp.roll(k_all, half_sides, axis=0).transpose(1, 0, 2, 3, 4).reshape(prompt_shape)
    v_prompt = jnp.roll(v_all, half_sides, axis=0).transpose(1, 0, 2, 3, 4).reshape(prompt_shape)
    dec_out, k_cache_new, v_cache_new = decode_rows(dec_tokens, k_cache, v_cache, c_len, w_qkv_dec, w_out_dec, w_gu_dec, w_down_dec, gain_dec)
    return (final_hidden.reshape(SIDES * PROMPT, D), dec_out, k_prompt, v_prompt, k_cache_new, v_cache_new)
```

```python
import functools

import jax
import jax.numpy as jnp
import numpy as np
from jax import lax
from jax.experimental import pallas as pl
from jax.experimental.pallas import tpu as pltpu
from jax.sharding import PartitionSpec as P

EPSILON = 1e-6
THETA = 10000.0
MASKED = -1e30
D_BLOCK = 256
D_SLOTS = 6
F_BLOCK = 256
F_SLOTS = 3
N_BLOCK = 512
F32 = jnp.float32
BF16 = jnp.bfloat16


VMEM = pl.BlockSpec(memory_space=pltpu.VMEM)
SMEM = pl.BlockSpec(memory_space=pltpu.SMEM)
HBM = pl.BlockSpec(memory_space=pltpu.HBM)


def dot(lhs, rhs):
    return jnp.dot(lhs, rhs, preferred_element_type=F32)


def dot_nt(lhs, rhs):
    return lax.dot_general(lhs, rhs, (((1,), (1,)), ((), ())), preferred_element_type=F32)


def rms(values, gain):
    inv = lax.rsqrt(jnp.mean(values * values, axis=-1, keepdims=True) + EPSILON)
    return (values * inv * gain).astype(BF16)


def rope_rows(positions, head_dim):
    half = head_dim // 2
    inv_freq = np.power(np.float32(THETA), -np.arange(half, dtype=np.float32) * np.float32(2.0) / np.float32(head_dim)).astype(np.float32)
    angles = np.arange(positions, dtype=np.float32)[:, None] * inv_freq[None, :]
    cos_half = np.cos(angles).astype(np.float32)
    sin_half = np.sin(angles).astype(np.float32)
    return jnp.asarray(np.concatenate([cos_half, cos_half], 1)), jnp.asarray(np.concatenate([-sin_half, sin_half], 1))


def rotate(values, cos_b, sin_b):
    return values * cos_b + pltpu.roll(values, values.shape[-1] // 2, 1) * sin_b


def stream_qkv(n_ref, w_hbm, buf, sem, acc):
    width, kinds, heads, _ = w_hbm.shape
    steps = width // D_BLOCK

    def load(i, slot):
        return pltpu.make_async_copy(w_hbm.at[pl.ds(i * D_BLOCK, D_BLOCK)], buf.at[slot], sem.at[slot])

    acc[...] = jnp.zeros_like(acc)

    @pl.loop(0, steps)
    def _(i):
        @pl.when(i + D_SLOTS - 1 < steps)
        def _():
            load(i + D_SLOTS - 1, lax.rem(i + D_SLOTS - 1, D_SLOTS)).start()
        slot = lax.rem(i, D_SLOTS)
        load(i, slot).wait()
        nb = n_ref[:, pl.ds(pl.multiple_of(i * D_BLOCK, D_BLOCK), D_BLOCK)]
        for kind in range(kinds):
            by_head = jnp.swapaxes(buf[slot, :, kind], 0, 1)
            for p in range(heads // 2):
                pair = jnp.concatenate([by_head[2 * p], by_head[2 * p + 1]], axis=1)
                acc[kind * (heads // 2) + p] += dot(nb, pair)


def start_qkv(w_hbm, buf, sem):
    for slot in range(D_SLOTS - 1):
        pltpu.make_async_copy(w_hbm.at[pl.ds(slot * D_BLOCK, D_BLOCK)], buf.at[slot], sem.at[slot]).start()


def split_rows(part, cols, outs):
    send_a, keep_a, send_b, keep_b = outs
    q = part.shape[0] // 8
    piece = [part[i * q:(i + 1) * q] for i in range(8)]
    send_a[0, :, cols], send_a[1, :, cols] = piece[2], piece[4]
    keep_a[0, :, cols], keep_a[1, :, cols] = piece[0], piece[6]
    send_b[0, :, cols], send_b[1, :, cols] = piece[7], piece[5]
    keep_b[0, :, cols], keep_b[1, :, cols] = piece[1], piece[3]


def prefill_attn_kernel(s_len, y_ref, x_ref, g_ref, cos_ref, sin_ref, w_hbm, wo_hbm, *rest):
    outs, kv_out = rest[:4], rest[4:8]
    buf, sem, wo_buf, wo_sem, n_ref, acc, ctx, ctx_rel, k_scr, v_scr = rest[8:]
    rows, width = x_ref.shape
    heads, head = w_hbm.shape[2], w_hbm.shape[3]
    pairs = heads // 2
    start_qkv(w_hbm, buf, sem)
    wo_copy = pltpu.make_async_copy(wo_hbm, wo_buf, wo_sem)
    wo_copy.start()

    @pl.loop(0, rows // 16)
    def _(i):
        r = pl.ds(pl.multiple_of(i * 16, 16), 16)
        n_ref[r, :] = rms(x_ref[r, :].astype(F32), g_ref[...])

    stream_qkv(n_ref, w_hbm, buf, sem, acc)
    cos_b, sin_b = cos_ref[...], sin_ref[...]
    row_id = lax.broadcasted_iota(jnp.int32, (rows, rows), 0)
    col_id = lax.broadcasted_iota(jnp.int32, (rows, rows), 1)
    allowed = (col_id <= row_id) & (col_id < s_len[0])

    @pl.loop(0, pairs)
    def _(p):
        pair_ctx = []
        for side in range(2):
            lanes = slice(side * head, (side + 1) * head)
            q = rotate(acc[p, :, lanes], cos_b, sin_b).astype(BF16)
            k = rotate(acc[pairs + p, :, lanes], cos_b, sin_b).astype(BF16)
            v = acc[2 * pairs + p, :, lanes].astype(BF16)
            k_scr[2 * p + side] = k
            v_scr[2 * p + side] = v
            scores = jnp.where(allowed, dot_nt(q, k) * head ** -0.5, MASKED)
            top = jnp.max(scores, axis=-1, keepdims=True)
            weights = jnp.exp(scores - top)
            prob = (weights / jnp.sum(weights, axis=-1, keepdims=True)).astype(BF16)
            pair_ctx.append(dot(prob, v).astype(BF16))
        ctx[:, pl.ds(pl.multiple_of(p * 2 * head, 2 * head), 2 * head)] = jnp.concatenate(pair_ctx, axis=1)

    y = y_ref[0]
    block = rows // 4
    for r in range(4):
        owner = lax.bitwise_xor(y, r)
        ctx_rel[r * block:(r + 1) * block, :] = ctx[pl.ds(pl.multiple_of(owner * block, block), block), :]
        for jj in range(heads // 4):
            kv_out[r][0, jj] = k_scr[jj * 4 + owner]
            kv_out[r][1, jj] = v_scr[jj * 4 + owner]
    wo_copy.wait()
    lhs = ctx_rel[...]
    for c in range(width // N_BLOCK):
        cols = slice(c * N_BLOCK, (c + 1) * N_BLOCK)
        split_rows(dot(lhs, wo_buf[:, cols]), cols, outs)


def decode_qkv_kernel(c_len, x_ref, g_ref, cos_ref, sin_ref, w_hbm, q_ref, k_ref, v_ref, buf, sem, n_ref, acc):
    rows, width = x_ref.shape
    heads, head = w_hbm.shape[2], w_hbm.shape[3]
    pairs = heads // 2
    start_qkv(w_hbm, buf, sem)
    n_ref[...] = rms(x_ref[...].astype(F32), g_ref[...])
    stream_qkv(n_ref, w_hbm, buf, sem, acc)
    cos_b = jnp.concatenate([cos_ref[pl.ds(c_len[b], 1), :] for b in range(rows)], axis=0)
    sin_b = jnp.concatenate([sin_ref[pl.ds(c_len[b], 1), :] for b in range(rows)], axis=0)

    def by_row(kind, turn):
        found = []
        for h in range(heads):
            vals = acc[kind * pairs + h // 2, :, (h % 2) * head:(h % 2 + 1) * head]
            found.append(rotate(vals, cos_b, sin_b) if turn else vals)
        return jnp.swapaxes(jnp.stack(found), 0, 1).astype(BF16)

    q_ref[...] = by_row(0, True)
    k_ref[...] = by_row(1, True)
    v_ref[...] = by_row(2, False)


def decode_attn_kernel(c_len, y_ref, q_ref, k_ref, v_ref, kc_ref, vc_ref, wo_hbm, part_ref, kn_ref, vn_ref, ctx, wo_buf, wo_sem, part_scr):
    b = pl.program_id(0)
    heads, head = q_ref.shape[1], q_ref.shape[2]
    wo_copy = pltpu.make_async_copy(wo_hbm, wo_buf, wo_sem)

    @pl.when(b == 0)
    def _():
        wo_copy.start()

    clen = c_len[b]
    q = q_ref[0].astype(F32)
    k_tok, v_tok = k_ref[0], v_ref[0]
    scale = head ** -0.5
    kc = kc_ref[0]
    scores = jnp.sum(kc.astype(F32) * q[None], axis=-1, keepdims=True) * scale
    t_id = lax.broadcasted_iota(jnp.int32, scores.shape, 0)
    scores = jnp.where(t_id < clen, scores, MASKED)
    own = jnp.sum(q * k_tok.astype(F32), axis=-1, keepdims=True) * scale
    top = jnp.maximum(jnp.max(scores, axis=0), own)
    weights = jnp.exp(scores - top[None])
    own_w = jnp.exp(own - top)
    total = jnp.sum(weights, axis=0) + own_w
    prob = (weights / total[None]).astype(BF16).astype(F32)
    own_prob = (own_w / total).astype(BF16).astype(F32)
    vc = vc_ref[0]
    context = jnp.sum(prob * vc.astype(F32), axis=0) + own_prob * v_tok.astype(F32)
    ctx[b] = context.astype(BF16).astype(F32)
    kn_ref[0] = kc
    vn_ref[0] = vc
    kn_ref[0, clen] = k_tok
    vn_ref[0, clen] = v_tok

    @pl.when(b == pl.num_programs(0) - 1)
    def _():
        by_head = jnp.swapaxes(ctx[...], 0, 1)
        lhs = jnp.concatenate([by_head[h] for h in range(heads)], axis=1).astype(BF16)
        wo_copy.wait()
        width = wo_buf.shape[1]
        for c in range(4):
            part_scr[c] = dot(lhs, wo_buf[:, c * (width // 4):(c + 1) * (width // 4)])
        for r in range(4):
            part_ref[r] = part_scr[lax.bitwise_xor(y_ref[0], r)]


def stream_mlp(n_ref, gu_hbm, down_hbm, bufs, sem, first, last, add):
    ff = down_hbm.shape[0]
    width = down_hbm.shape[1]
    g_buf, u_buf, d_buf = bufs

    def at(i):
        return pl.multiple_of(jnp.minimum(i * F_BLOCK, ff - F_BLOCK), 8)

    def loads(i):
        slot = lax.rem(i - first, F_SLOTS)
        rows = pl.ds(at(i), F_BLOCK)
        return (pltpu.make_async_copy(gu_hbm.at[0, rows], g_buf.at[slot], sem.at[0, slot]),
                pltpu.make_async_copy(gu_hbm.at[1, rows], u_buf.at[slot], sem.at[1, slot]),
                pltpu.make_async_copy(down_hbm.at[rows], d_buf.at[slot], sem.at[2, slot]))

    def begin():
        for i in range(first, min(first + F_SLOTS - 1, last)):
            for copy in loads(i):
                copy.start()

    def run():
        @pl.loop(first, last)
        def _(i):
            @pl.when(i + F_SLOTS - 1 < last)
            def _():
                for copy in loads(i + F_SLOTS - 1):
                    copy.start()
            slot = lax.rem(i - first, F_SLOTS)
            for copy in loads(i):
                copy.wait()
            n = n_ref[...]
            gate = dot_nt(n, g_buf[slot]).astype(BF16).astype(F32)
            up = dot_nt(n, u_buf[slot]).astype(BF16).astype(F32)
            m = jax.nn.silu(gate) * up
            lane = lax.broadcasted_iota(jnp.int32, m.shape, 1)
            m = jnp.where(at(i) + lane >= i * F_BLOCK, m, 0.0).astype(BF16)
            for c in range(width // N_BLOCK):
                cols = slice(c * N_BLOCK, (c + 1) * N_BLOCK)
                add(dot(m, d_buf[slot, :, cols]), cols)

    return begin, run


def prefill_mlp_kernel(n0, n1, n2, n3, gu_hbm, down_hbm, send_a, keep_a, send_b, keep_b, g_buf, u_buf, d_buf, sem, n_ref):
    outs = (send_a, keep_a, send_b, keep_b)

    def add(part, cols):
        q = part.shape[0] // 8
        piece = [part[i * q:(i + 1) * q] for i in range(8)]
        for ref, first, second in ((send_a, 2, 4), (keep_a, 0, 6), (send_b, 7, 5), (keep_b, 1, 3)):
            ref[0, :, cols] += piece[first]
            ref[1, :, cols] += piece[second]

    ff = down_hbm.shape[0]
    begin, run = stream_mlp(n_ref, gu_hbm, down_hbm, (g_buf, u_buf, d_buf), sem, 0, pl.cdiv(ff, F_BLOCK), add)
    begin()
    block = n0.shape[0]
    for r, ref in enumerate((n0, n1, n2, n3)):
        n_ref[r * block:(r + 1) * block, :] = ref[...]
    for ref in outs:
        ref[...] = jnp.zeros_like(ref)
    run()


def decode_mlp_kernel(first, last, y_ref, x_ref, g_ref, a0, a1, a2, a3, prev_ref, gu_hbm, down_hbm, part_ref, g_buf, u_buf, d_buf, sem, n_ref, h_ref, part_scr):
    quarter = a0.shape[1]

    def add(part, cols):
        c = cols.start // quarter
        part_scr[c, :, cols.start - c * quarter:cols.stop - c * quarter] += part

    begin, run = stream_mlp(n_ref, gu_hbm, down_hbm, (g_buf, u_buf, d_buf), sem, first, last, add)
    begin()
    y = y_ref[0]
    for r, ref in enumerate((a0, a1, a2, a3)):
        owner = lax.bitwise_xor(y, r)
        cols = pl.ds(pl.multiple_of(owner * quarter, quarter), quarter)
        h_ref[:, cols] = x_ref[:, cols].astype(F32) + ref[...].astype(F32)
        part_scr[owner] = prev_ref[r]
    n_ref[...] = rms(h_ref[...].astype(BF16).astype(F32), g_ref[...])
    run()
    for r in range(4):
        part_ref[r] = part_scr[lax.bitwise_xor(y, r)]


def own_rows_kernel(y_ref, ka, ra, sa, kb, rb, sb, x_ref, g_ref, h_ref, n_ref):
    q = ka.shape[1]
    for at, keep, got, second in ((0, ka, ra, sa), (q, kb, rb, sb)):
        total = (keep[0] + got[0]) + second[...]
        rows = slice(at, at + q)
        h = (x_ref[rows, :].astype(F32) + total.astype(BF16).astype(F32)).astype(BF16)
        h_ref[rows, :] = h
        n_ref[rows, :] = rms(h.astype(F32), g_ref[...])


def place_rows_kernel(y_ref, h0, h1, h2, h3, out_hbm, sem):
    block = h0.shape[0]
    copies = []
    for r, ref in enumerate((h0, h1, h2, h3)):
        owner = lax.bitwise_xor(y_ref[0], r)
        copies.append(pltpu.make_async_copy(ref, out_hbm.at[pl.ds(pl.multiple_of(owner * block, block), block)], sem.at[r]))
    for copy in copies:
        copy.start()
    for copy in copies:
        copy.wait()


def place_kv_kernel(y_ref, r0, r1, r2, r3, k_ref, v_ref, k_scr, v_scr):
    per = r0.shape[1]
    for r, ref in enumerate((r0, r1, r2, r3)):
        owner = lax.bitwise_xor(y_ref[0], r)
        for jj in range(per):
            k_scr[owner * per + jj] = ref[0, jj]
            v_scr[owner * per + jj] = ref[1, jj]
    k_ref[...] = jnp.swapaxes(k_scr[...], 0, 1)
    v_ref[...] = jnp.swapaxes(v_scr[...], 0, 1)


def call(kernel, name, in_specs, out_specs, out_shape, scratch, us, **more):
    return pl.pallas_call(kernel, name=name, in_specs=in_specs, out_specs=out_specs, out_shape=out_shape, scratch_shapes=scratch,
                          cost_estimate=pl.CostEstimate(flops=int(us * 2e7), bytes_accessed=int(us * 3e6), transcendentals=0),
                          compiler_params=pltpu.CompilerParams(vmem_limit_bytes=60 * 2 ** 20), **more)


def shape(dims, dtype=F32):
    return jax.ShapeDtypeStruct(dims, dtype)


def after(values, *firsts):
    return lax.optimization_barrier((values,) + firsts)[0]


def solution(mesh):
    tp = mesh.shape['tp']
    side = mesh.shape['side']
    inst_axes = ('pair', 'side')
    rows_spec = P(inst_axes, None)
    vec_spec = P(inst_axes)
    cache_spec = P(None, inst_axes, None, None, 'tp', None)
    prompt_spec = P(None, inst_axes, None, 'tp', None)
    in_specs = (rows_spec, vec_spec, P(None, None, None, 'tp', None), P(None, 'tp', None, None), P(None, None, 'tp', None), P(None, 'tp', None), P(None, None, None), rows_spec, cache_spec, cache_spec, vec_spec, P(None, None, None, None, 'tp', None), P(None, None, 'tp', None, None), P(None, None, 'tp', None), P(None, 'tp', None), P(None, None, None))
    out_specs = (rows_spec, rows_spec, prompt_spec, prompt_spec, cache_spec, cache_spec)

    def swap(value, r):
        return lax.ppermute(value, 'tp', [(i, i ^ r) for i in range(tp)])

    def swap_far(value, r):
        perm = [(t * side + s, (t ^ r) * side + (s + side // 2) % side) for t in range(tp) for s in range(side)]
        return lax.ppermute(value, ('tp', 'side'), perm)

    def device_fn(prompt_x, s_len, w_qkv_pre, w_out_pre, w_gu_pre, w_down_pre, gain_pre, dec_tokens, k_cache, v_cache, c_len, w_qkv_dec, w_out_dec, w_gu_dec, w_down_dec, gain_dec):
        rows, width = prompt_x.shape
        batch = dec_tokens.shape[0]
        heads, head = w_qkv_pre.shape[3], w_qkv_pre.shape[4]
        cache_len = k_cache.shape[2]
        ff = w_down_pre.shape[1]
        piece = rows // 8
        quarter = width // 4
        y = lax.axis_index('tp').astype(jnp.int32)[None]
        cos_tab, sin_tab = rope_rows(max(rows, cache_len), head)
        qkv_buf = [pltpu.VMEM((D_SLOTS, D_BLOCK, 3, heads, head), BF16), pltpu.SemaphoreType.DMA((D_SLOTS,))]
        wo_scr = [pltpu.VMEM((heads * head, width), BF16), pltpu.SemaphoreType.DMA]
        mlp_buf = [pltpu.VMEM((F_SLOTS, F_BLOCK, width), BF16)] * 3 + [pltpu.SemaphoreType.DMA((3, F_SLOTS))]
        split_shapes = [shape((2, piece, width))] * 4

        attn = call(prefill_attn_kernel, 'prefill_attn', [SMEM, SMEM] + [VMEM] * 4 + [HBM] * 2, [VMEM] * 8,
                    split_shapes + [shape((2, heads // 4, rows, head), BF16)] * 4,
                    qkv_buf + wo_scr + [pltpu.VMEM((rows, width), BF16), pltpu.VMEM((3 * heads // 2, rows, 2 * head), F32), pltpu.VMEM((rows, heads * head), BF16), pltpu.VMEM((rows, heads * head), BF16), pltpu.VMEM((heads, rows, head), BF16), pltpu.VMEM((heads, rows, head), BF16)], 18)(
            s_len, y, prompt_x, gain_pre[0, 0:1], cos_tab[:rows], sin_tab[:rows], w_qkv_pre[0], w_out_pre.reshape(heads * head, width))
        send_a, keep_a, send_b, keep_b = attn[:4]
        got_a, got_b = swap(send_a, 1), swap(send_b, 3)
        far = [swap_far(value, r) for r, value in enumerate(attn[4:])]

        tokens = after(dec_tokens, keep_a)
        q, k_tok, v_tok = call(decode_qkv_kernel, 'decode_qkv', [SMEM] + [VMEM] * 4 + [HBM], [VMEM] * 3, [shape((batch, heads, head), BF16)] * 3,
                               qkv_buf + [pltpu.VMEM((batch, width), BF16), pltpu.VMEM((3 * heads // 2, batch, 2 * head), F32)], 12)(
            c_len, tokens, gain_dec[0, 0:1], cos_tab, sin_tab, w_qkv_dec.reshape(width, 3, heads, head))

        got_a, got_b, q = lax.optimization_barrier((got_a, got_b, q))
        second_a, second_b = swap(keep_a[1] + got_a[1], 3), swap(keep_b[1] + got_b[1], 1)

        row_block = pl.BlockSpec((1, heads, head), lambda b: (b, 0, 0))
        cache_block = pl.BlockSpec((1, cache_len, heads, head), lambda b: (b, 0, 0, 0))
        cache_shape = (batch, cache_len, heads, head)
        d_part, k_new, v_new = call(decode_attn_kernel, 'decode_attn', [SMEM, SMEM] + [row_block] * 3 + [cache_block] * 2 + [HBM],
                                    [pl.BlockSpec((4, batch, quarter), lambda b: (0, 0, 0)), cache_block, cache_block],
                                    [shape((4, batch, quarter)), shape(cache_shape, BF16), shape(cache_shape, BF16)],
                                    [pltpu.VMEM((batch, heads, head), F32)] + wo_scr + [pltpu.VMEM((4, batch, quarter), F32)], 10, grid=(batch,))(
            c_len, y, q, k_tok, v_tok, k_cache.reshape(cache_shape), v_cache.reshape(cache_shape), w_out_dec.reshape(heads * head, width))

        def reduce_cols(part):
            total = (part[0] + swap(part[1], 1)) + (swap(part[2], 2) + swap(part[3], 3))
            return total.astype(BF16)

        second_a, second_b, d_part = lax.optimization_barrier((second_a, second_b, d_part))
        block = 2 * piece
        whole = pl.BlockSpec((2, piece, width), lambda i, y_ref: (0, 0, 0))
        flat = pl.BlockSpec((piece, width), lambda i, y_ref: (0, 0))
        mine = pl.BlockSpec((block, width), lambda i, y_ref: (y_ref[0], 0))
        own = pl.BlockSpec((block, width), lambda i, y_ref: (0, 0))
        h_own, n_own = pl.pallas_call(
            own_rows_kernel, name='own_rows', out_shape=[shape((block, width), BF16)] * 2,
            grid_spec=pltpu.PrefetchScalarGridSpec(num_scalar_prefetch=1, grid=(1,), in_specs=[whole, whole, flat, whole, whole, flat, mine, pl.BlockSpec((1, width), lambda i, y_ref: (0, 0))], out_specs=[own, own]),
            cost_estimate=pl.CostEstimate(flops=2 * 10 ** 7, bytes_accessed=10 ** 6, transcendentals=0))(
            y, keep_a, got_a, second_a, keep_b, got_b, second_b, prompt_x, gain_pre[0, 1:2])
        n_all = [n_own] + [swap(n_own, r) for r in (1, 2, 3)]

        a_own = reduce_cols(d_part)
        a_all = [a_own] + [swap(a_own, r) for r in (1, 2, 3)]
        steps = -(-ff // F_BLOCK)

        def decode_mlp(first, last, a_all, prev):
            return call(functools.partial(decode_mlp_kernel, first, last), 'decode_mlp', [SMEM] + [VMEM] * 7 + [HBM] * 2, VMEM, shape((4, batch, quarter)),
                        mlp_buf + [pltpu.VMEM((batch, width), BF16), pltpu.VMEM((batch, width), F32), pltpu.VMEM((4, batch, quarter), F32)], 2 * (last - first))(
                y, dec_tokens, gain_dec[0, 1:2], *a_all, prev, w_gu_dec[0], w_down_dec[0])

        cut_1, cut_2 = 4, 9
        d_part = decode_mlp(0, cut_1, a_all, jnp.zeros((4, batch, quarter), F32))
        n_all, d_part = lax.optimization_barrier((n_all, d_part))
        send_a, keep_a, send_b, keep_b = call(prefill_mlp_kernel, 'prefill_mlp', [VMEM] * 4 + [HBM] * 2, [VMEM] * 4, split_shapes,
                                              mlp_buf + [pltpu.VMEM((rows, width), BF16)], 22)(*n_all, w_gu_pre[0], w_down_pre[0])
        got_a, got_b = swap(send_a, 1), swap(send_b, 3)
        d_part = after(d_part, keep_a)
        d_part = decode_mlp(cut_1, cut_2, a_all, d_part)
        got_a, got_b, d_part = lax.optimization_barrier((got_a, got_b, d_part))
        second_a, second_b = swap(keep_a[1] + got_a[1], 3), swap(keep_b[1] + got_b[1], 1)
        d_part = decode_mlp(cut_2, steps, a_all, d_part)

        second_a, second_b, d_part = lax.optimization_barrier((second_a, second_b, d_part))
        total = jnp.concatenate([keep_a[0] + got_a[0] + second_a, keep_b[0] + got_b[0] + second_b], axis=0)
        out_own = (h_own.astype(F32) + total.astype(BF16).astype(F32)).astype(BF16)
        out_all = [out_own] + [swap(out_own, r) for r in (1, 2, 3)]

        d_own = reduce_cols(d_part)
        cols = (0, y[0] * quarter)
        tok_own = lax.dynamic_slice(dec_tokens, cols, (batch, quarter))
        h_dec = (tok_own.astype(F32) + a_own.astype(F32)).astype(BF16)
        dec_own = (h_dec.astype(F32) + d_own.astype(F32)).astype(BF16)
        dec_all = [dec_own] + [swap(dec_own, r) for r in (1, 2, 3)]
        dec_out = jnp.zeros((batch, width), BF16)
        for r in range(4):
            dec_out = lax.dynamic_update_slice(dec_out, dec_all[r], (0, (y[0] ^ r) * quarter))

        far, d_part = lax.optimization_barrier((far, d_part))
        k_prompt, v_prompt = call(place_kv_kernel, 'place_kv', [SMEM] + [VMEM] * 4, [VMEM] * 2, [shape((rows, heads, head), BF16)] * 2,
                                  [pltpu.VMEM((heads, rows, head), BF16)] * 2, 2)(y, *far)
        out_all, k_prompt = lax.optimization_barrier((out_all, k_prompt))
        h_out = call(place_rows_kernel, 'place_rows', [SMEM] + [VMEM] * 4, HBM, shape((rows, width), BF16), [pltpu.SemaphoreType.DMA((4,))], 2)(y, *out_all)
        prompt_shape = (1, rows, heads, 1, head)
        return h_out, dec_out, k_prompt.reshape(prompt_shape), v_prompt.reshape(prompt_shape), k_new.reshape(k_cache.shape), v_new.reshape(v_cache.shape)

    return jax.shard_map(device_fn, mesh=mesh, in_specs=in_specs, out_specs=out_specs, check_vma=False)
```

```python
import functools

import jax
import jax.numpy as jnp
import numpy as np
from jax import lax
from jax.experimental import pallas as pl
from jax.experimental.pallas import tpu as pltpu
from jax.sharding import PartitionSpec as P

EPSILON = 1e-6
THETA = 10000.0
MASKED = -1e30
D_BLOCK = 512
D_SLOTS = 4
F_BLOCK = 256
F_SLOTS = 3
N_BLOCK = 512
GROUPS = 2
F32 = jnp.float32
BF16 = jnp.bfloat16

MESH = pl.DeviceIdType.MESH

VMEM = pl.BlockSpec(memory_space=pltpu.VMEM)
SMEM = pl.BlockSpec(memory_space=pltpu.SMEM)
HBM = pl.BlockSpec(memory_space=pltpu.HBM)


def dot(lhs, rhs):
    return jnp.dot(lhs, rhs, preferred_element_type=F32)


def dot_nt(lhs, rhs):
    return lax.dot_general(lhs, rhs, (((1,), (1,)), ((), ())), preferred_element_type=F32)


def rms(values, gain):
    inv = lax.rsqrt(jnp.mean(values * values, axis=-1, keepdims=True) + EPSILON)
    return (values * inv * gain).astype(BF16)


def rope_rows(positions, head_dim):
    half = head_dim // 2
    inv_freq = np.power(np.float32(THETA), -np.arange(half, dtype=np.float32) * np.float32(2.0) / np.float32(head_dim)).astype(np.float32)
    angles = np.arange(positions, dtype=np.float32)[:, None] * inv_freq[None, :]
    cos_half = np.cos(angles).astype(np.float32)
    sin_half = np.sin(angles).astype(np.float32)
    return jnp.asarray(np.concatenate([cos_half, cos_half], 1)), jnp.asarray(np.concatenate([-sin_half, sin_half], 1))


def rotate(values, cos_b, sin_b):
    return values * cos_b + pltpu.roll(values, values.shape[-1] // 2, 1) * sin_b


def qkv_product(n_ref, block, at, acc):
    kinds, heads = block.shape[1], block.shape[2]
    nb = n_ref[:, pl.ds(pl.multiple_of(at * D_BLOCK, D_BLOCK), D_BLOCK)]
    for kind in range(kinds):
        by_head = jnp.swapaxes(block[:, kind], 0, 1)
        for p in range(heads // 2):
            pair = jnp.concatenate([by_head[2 * p], by_head[2 * p + 1]], axis=1)
            acc[kind * (heads // 2) + p] += dot(nb, pair)


def remote(src, dst, send_sem, recv_sem, where):
    return pltpu.make_async_remote_copy(src_ref=src, dst_ref=dst, send_sem=send_sem, recv_sem=recv_sem, device_id=where, device_id_type=MESH)


def greet(peers):
    barrier = pltpu.get_barrier_semaphore()
    for peer in peers:
        pl.semaphore_signal(barrier, inc=1, device_id=peer, device_id_type=MESH)


def greeted(peers):
    pl.semaphore_wait(pltpu.get_barrier_semaphore(), len(peers))


class RowReduce:
    def __init__(self, y, refs):
        (self.send_a, self.keep_a, self.send_b, self.keep_b, self.got_a, self.got_b,
         self.mid_a, self.mid_b, self.fin_a, self.fin_b, self.s_sem, self.r_sem) = refs
        self.near = {'tp': lax.bitwise_xor(y, 1)}
        self.wrap = {'tp': lax.bitwise_xor(y, 3)}

    @staticmethod
    def scratch(piece, width):
        part = width // GROUPS
        two, one = pltpu.VMEM((GROUPS, 2, piece, part), F32), pltpu.VMEM((GROUPS, piece, part), F32)
        return [two] * 6 + [one] * 4 + [pltpu.SemaphoreType.DMA((2, 2, GROUPS))] * 2

    def first(self, c):
        return (remote(self.send_a.at[c], self.got_a.at[c], self.s_sem.at[0, 0, c], self.r_sem.at[0, 0, c], self.near),
                remote(self.send_b.at[c], self.got_b.at[c], self.s_sem.at[0, 1, c], self.r_sem.at[0, 1, c], self.wrap))

    def second(self, c):
        return (remote(self.mid_a.at[c], self.fin_a.at[c], self.s_sem.at[1, 0, c], self.r_sem.at[1, 0, c], self.wrap),
                remote(self.mid_b.at[c], self.fin_b.at[c], self.s_sem.at[1, 1, c], self.r_sem.at[1, 1, c], self.near))

    def put(self, part, cols, add):
        q = part.shape[0] // 8
        piece = [part[i * q:(i + 1) * q] for i in range(8)]
        size = self.send_a.shape[-1]
        c = cols.start // size
        at = slice(cols.start - c * size, cols.stop - c * size)
        for ref, one, two in ((self.send_a, 2, 4), (self.keep_a, 0, 6), (self.send_b, 7, 5), (self.keep_b, 1, 3)):
            for row, i in ((0, one), (1, two)):
                ref[c, row, :, at] = ref[c, row, :, at] + piece[i] if add else piece[i]

    def start(self, c):
        for copy in self.first(c):
            copy.start()

    def middle(self, c):
        for copy, keep, got, mid, after in zip(self.first(c), (self.keep_a, self.keep_b), (self.got_a, self.got_b), (self.mid_a, self.mid_b), self.second(c)):
            copy.wait_recv()
            mid[c] = keep[c, 1] + got[c, 1]
            after.start()

    def totals(self):
        found = []
        for i, (keep, got, fin) in enumerate(((self.keep_a, self.got_a, self.fin_a), (self.keep_b, self.got_b, self.fin_b))):
            cols = []
            for c in range(GROUPS):
                self.second(c)[i].wait_recv()
                cols.append((keep[c, 0] + got[c, 0]) + fin[c])
            found.append(jnp.concatenate(cols, axis=1))
        return found

    def drain(self):
        for c in range(GROUPS):
            for copy in self.first(c) + self.second(c):
                copy.wait_send()


class RowGather:
    def __init__(self, y, rows, s_sem, r_sem):
        near, wrap = {'tp': lax.bitwise_xor(y, 1)}, {'tp': lax.bitwise_xor(y, 3)}
        moves = ((0, 0, 3, 0, wrap), (0, 1, 1, 1, near), (0, 0, 1, 0, near), (0, 1, 3, 1, wrap), (3, 0, 2, 0, near), (1, 1, 2, 1, wrap))
        self.copies = [remote(rows.at[r, h], rows.at[to, h2], s_sem.at[i], r_sem.at[i], where) for i, (r, h, to, h2, where) in enumerate(moves)]

    @staticmethod
    def scratch(piece, width):
        return [pltpu.VMEM((4, 2, piece, width), BF16)] + [pltpu.SemaphoreType.DMA((6,))] * 2

    def start(self):
        for copy in self.copies[:4]:
            copy.start()

    def forward(self):
        for i in range(2):
            self.copies[i].wait_recv()
            self.copies[4 + i].start()

    def finish(self):
        for copy in self.copies[2:]:
            copy.wait_recv()
        for copy in self.copies:
            copy.wait_send()


class ColumnSum:
    def __init__(self, y, refs):
        self.y = y
        self.part, self.got, self.total, self.s_sem, self.r_sem = refs

    @staticmethod
    def scratch(batch, quarter):
        return [pltpu.VMEM((4, batch, quarter), F32), pltpu.VMEM((4, batch, quarter), F32), pltpu.VMEM((4, batch, quarter), BF16)] + [pltpu.SemaphoreType.DMA((2, 4))] * 2

    def copies(self, step):
        src, dst = ((self.part, self.got), (self.total, self.total))[step]
        return [remote(src.at[0 if step else r], dst.at[r], self.s_sem.at[step, r], self.r_sem.at[step, r], {'tp': lax.bitwise_xor(self.y, r)}) for r in (1, 2, 3)]

    def start(self):
        for copy in self.copies(0):
            copy.start()

    def middle(self):
        for copy in self.copies(0):
            copy.wait_recv()
        self.total[0] = ((self.part[0] + self.got[1]) + (self.got[2] + self.got[3])).astype(BF16)
        for copy in self.copies(1):
            copy.start()

    def finish(self, out_ref):
        for copy in self.copies(1):
            copy.wait_recv()
        quarter = self.total.shape[-1]
        for r in range(4):
            owner = lax.bitwise_xor(self.y, r)
            out_ref[:, pl.ds(pl.multiple_of(owner * quarter, quarter), quarter)] = self.total[r].astype(out_ref.dtype)
        for step in range(2):
            for copy in self.copies(step):
                copy.wait_send()


def attn_kernel(side, s_len, c_len, x_ref, g_ref, cos_ref, sin_ref, tok_ref, dg_ref, wp_hbm, wop_hbm, wd_hbm, kc_hbm, vc_hbm, wod_hbm,
                h_ref, n_out, a_ref, kt_ref, vt_ref, kp_ref, vp_ref,
                buf, sem, wo_buf, wo_sem, cache, cache_sem, n_ref, acc, ctx, ctx_rel, k_scr, v_scr, nd_ref, accd, q_scr, ctxd, part_scr,
                kv_send, kv_got, kv_ssem, kv_rsem, *comm):
    y = lax.axis_index('tp')
    s = lax.axis_index('side')
    far = lax.rem(s + side // 2, side)
    near_peers = [{'tp': lax.bitwise_xor(y, r)} for r in (1, 2, 3)]
    far_peers = [{'tp': lax.bitwise_xor(y, r), 'side': far} for r in range(4)]
    reduce = RowReduce(y, comm[:12])
    rows_all = comm[12]
    gather = RowGather(y, *comm[12:15])
    small = ColumnSum(y, comm[15:20])
    rows, width = x_ref.shape
    batch = tok_ref.shape[0]
    heads, head = wp_hbm.shape[2], wp_hbm.shape[3]
    pairs = heads // 2
    steps = width // D_BLOCK
    scale = head ** -0.5

    def load(i, w_hbm, slot):
        return pltpu.make_async_copy(w_hbm.at[pl.ds(i * D_BLOCK, D_BLOCK)], buf.at[slot], sem.at[slot])

    def wo_load(which):
        return pltpu.make_async_copy((wop_hbm, wod_hbm)[which], wo_buf.at[which], wo_sem.at[which])

    def cache_load(b, which):
        return pltpu.make_async_copy((kc_hbm, vc_hbm)[which].at[b], cache.at[which, b], cache_sem.at[which, b])

    for i in range(D_SLOTS - 1):
        load(i, wp_hbm, i).start()
    greet(near_peers + far_peers)

    @pl.loop(0, rows // 16)
    def _(i):
        r = pl.ds(pl.multiple_of(i * 16, 16), 16)
        n_ref[r, :] = rms(x_ref[r, :].astype(F32), g_ref[0:1, :])

    acc[...] = jnp.zeros_like(acc)
    accd[...] = jnp.zeros_like(accd)

    @pl.loop(0, steps)
    def _(i):
        j = i + D_SLOTS - 1

        @pl.when(j < steps)
        def _():
            load(j, wp_hbm, lax.rem(j, D_SLOTS)).start()

        @pl.when(j >= steps)
        def _():
            load(j - steps, wd_hbm, lax.rem(j, D_SLOTS)).start()

        @pl.when(i == 3)
        def _():
            wo_load(0).start()

        slot = lax.rem(i, D_SLOTS)
        load(i, wp_hbm, slot).wait()
        qkv_product(n_ref, buf.at[slot], i, acc)

    @pl.loop(0, batch)
    def _(b):
        cache_load(b, 0).start()
        cache_load(b, 1).start()

    cos_b, sin_b = cos_ref[:rows, :], sin_ref[:rows, :]
    row_id = lax.broadcasted_iota(jnp.int32, (rows, rows), 0)
    col_id = lax.broadcasted_iota(jnp.int32, (rows, rows), 1)
    allowed = (col_id <= row_id) & (col_id < s_len[0])

    @pl.loop(0, pairs)
    def _(p):
        pair_ctx = []
        for half in range(2):
            lanes = slice(half * head, (half + 1) * head)
            q = rotate(acc[p, :, lanes], cos_b, sin_b).astype(BF16)
            k = rotate(acc[pairs + p, :, lanes], cos_b, sin_b).astype(BF16)
            v = acc[2 * pairs + p, :, lanes].astype(BF16)
            k_scr[2 * p + half] = k
            v_scr[2 * p + half] = v
            scores = jnp.where(allowed, dot_nt(q, k) * scale, MASKED)
            top = jnp.max(scores, axis=-1, keepdims=True)
            weights = jnp.exp(scores - top)
            prob = (weights / jnp.sum(weights, axis=-1, keepdims=True)).astype(BF16)
            pair_ctx.append(dot(prob, v).astype(BF16))
        ctx[:, pl.ds(pl.multiple_of(p * 2 * head, 2 * head), 2 * head)] = jnp.concatenate(pair_ctx, axis=1)

    greeted(near_peers + far_peers)
    block = rows // 4
    for r in range(4):
        owner = lax.bitwise_xor(y, r)
        ctx_rel[r * block:(r + 1) * block, :] = ctx[pl.ds(pl.multiple_of(owner * block, block), block), :]
        for jj in range(heads // 4):
            kv_send[r, 0, jj] = k_scr[jj * 4 + owner]
            kv_send[r, 1, jj] = v_scr[jj * 4 + owner]
    kv_copies = [remote(kv_send.at[r], kv_got.at[r], kv_ssem.at[r], kv_rsem.at[r], far_peers[r]) for r in range(4)]
    wo_load(0).wait()
    lhs = ctx_rel[...]
    group = width // GROUPS
    for c in range(width // N_BLOCK):
        cols = slice(c * N_BLOCK, (c + 1) * N_BLOCK)
        reduce.put(dot(lhs, wo_buf[0, :, cols]), cols, False)
        if cols.stop % group == 0:
            reduce.start(cols.start // group)
    for copy in kv_copies:
        copy.start()

    wo_load(1).start()
    nd_ref[...] = rms(tok_ref[...].astype(F32), dg_ref[0:1, :])

    @pl.loop(0, steps)
    def _(i):
        j = i + D_SLOTS - 1

        @pl.when(j < steps)
        def _():
            load(j, wd_hbm, lax.rem(j + steps, D_SLOTS)).start()

        slot = lax.rem(i + steps, D_SLOTS)
        load(i, wd_hbm, slot).wait()
        qkv_product(nd_ref, buf.at[slot], i, accd)

        @pl.when(i == 4)
        def _():
            reduce.middle(0)

    cos_d = jnp.concatenate([cos_ref[pl.ds(c_len[b], 1), :] for b in range(batch)], axis=0)
    sin_d = jnp.concatenate([sin_ref[pl.ds(c_len[b], 1), :] for b in range(batch)], axis=0)

    def by_row(kind, turn):
        found = []
        for h in range(heads):
            vals = accd[kind * pairs + h // 2, :, (h % 2) * head:(h % 2 + 1) * head]
            found.append(rotate(vals, cos_d, sin_d) if turn else vals)
        return jnp.swapaxes(jnp.stack(found), 0, 1).astype(BF16)

    q_scr[...] = by_row(0, True)
    kt_ref[...] = by_row(1, True)
    vt_ref[...] = by_row(2, False)
    reduce.middle(1)
    slots = cache.shape[2]
    lane = lax.broadcasted_iota(jnp.int32, (heads, slots), 1)
    mine = lax.bitwise_and(lane, heads - 1) == lax.broadcasted_iota(jnp.int32, (heads, slots), 0)

    @pl.loop(0, batch)
    def _(b):
        cache_load(b, 0).wait()
        cache_load(b, 1).wait()
        q, k_tok, v_tok = q_scr[b], kt_ref[b].astype(F32), vt_ref[b].astype(F32)
        scores = dot_nt(q, cache[0, b]) * scale
        scores = jnp.where(mine & (lane < c_len[b] * heads), scores, MASKED)
        own = jnp.sum(q.astype(F32) * k_tok, axis=-1, keepdims=True) * scale
        top = jnp.maximum(jnp.max(scores, axis=-1, keepdims=True), own)
        weights = jnp.exp(scores - top)
        own_w = jnp.exp(own - top)
        total = jnp.sum(weights, axis=-1, keepdims=True) + own_w
        prob = (weights / total).astype(BF16)
        own_prob = (own_w / total).astype(BF16).astype(F32)
        ctxd[b] = (dot(prob, cache[1, b]) + own_prob * v_tok).astype(BF16).astype(F32)

    by_head = jnp.swapaxes(ctxd[...], 0, 1)
    lhs_d = jnp.concatenate([by_head[h] for h in range(heads)], axis=1).astype(BF16)
    wo_load(1).wait()
    quarter = width // 4
    for c in range(4):
        part_scr[c] = dot(lhs_d, wo_buf[1, :, c * quarter:(c + 1) * quarter])
    for r in range(4):
        small.part[r] = part_scr[lax.bitwise_xor(y, r)]
    small.start()

    piece = block // 2
    for at, total in zip((0, 1), reduce.totals()):
        x_rows = x_ref[pl.ds(pl.multiple_of(y * block + at * piece, piece), piece), :]
        h = (x_rows.astype(F32) + total.astype(BF16).astype(F32)).astype(BF16)
        h_ref[at * piece:(at + 1) * piece, :] = h
        rows_all[0, at] = rms(h.astype(F32), g_ref[1:2, :])
    gather.start()
    small.middle()
    for r in range(4):
        kv_copies[r].wait_recv()
        owner = lax.bitwise_xor(y, r)
        for jj in range(heads // 4):
            k_scr[owner * (heads // 4) + jj] = kv_got[r, 0, jj]
            v_scr[owner * (heads // 4) + jj] = kv_got[r, 1, jj]
    kp_ref[...] = jnp.swapaxes(k_scr[...], 0, 1)
    vp_ref[...] = jnp.swapaxes(v_scr[...], 0, 1)
    gather.forward()
    small.finish(a_ref)
    reduce.drain()
    for copy in kv_copies:
        copy.wait_send()
    gather.finish()
    n_out[...] = rows_all[...]


def mlp_kernel(n_all, own_ref, tok_ref, a_ref, dg_ref, gup_hbm, dnp_hbm, gud_hbm, dnd_hbm, h_out, d_out,
               g_buf, u_buf, d_buf, sem, n_ref, nd_ref, hd_ref, part_scr, *comm):
    y = lax.axis_index('tp')
    peers = [{'tp': lax.bitwise_xor(y, r)} for r in (1, 2, 3)]
    reduce = RowReduce(y, comm[:12])
    rows_all = comm[12]
    gather = RowGather(y, *comm[12:15])
    small = ColumnSum(y, comm[15:20])
    ff, width = dnp_hbm.shape
    steps = pl.cdiv(ff, F_BLOCK)
    quarter = width // 4

    def at(i):
        return pl.multiple_of(jnp.minimum(i * F_BLOCK, ff - F_BLOCK), 8)

    def loads(i, gu_hbm, down_hbm, slot):
        rows = pl.ds(at(i), F_BLOCK)
        return (pltpu.make_async_copy(gu_hbm.at[0, rows], g_buf.at[slot], sem.at[0, slot]),
                pltpu.make_async_copy(gu_hbm.at[1, rows], u_buf.at[slot], sem.at[1, slot]),
                pltpu.make_async_copy(down_hbm.at[rows], d_buf.at[slot], sem.at[2, slot]))

    def product(i, slot, n, add):
        gate = dot_nt(n, g_buf[slot]).astype(BF16).astype(F32)
        up = dot_nt(n, u_buf[slot]).astype(BF16).astype(F32)
        m = jax.nn.silu(gate) * up
        lane = lax.broadcasted_iota(jnp.int32, m.shape, 1)
        m = jnp.where(at(i) + lane >= i * F_BLOCK, m, 0.0).astype(BF16)
        for c in range(width // N_BLOCK):
            cols = slice(c * N_BLOCK, (c + 1) * N_BLOCK)
            add(dot(m, d_buf[slot, :, cols]), cols)

    for i in range(F_SLOTS - 1):
        for copy in loads(i, gup_hbm, dnp_hbm, i):
            copy.start()
    greet(peers)
    rows = n_ref.shape[0]
    piece = rows // 8
    for r in range(4):
        for half in range(2):
            i = (2 * r + half) * piece
            n_ref[i:i + piece, :] = n_all[r, half]
    for ref in (reduce.send_a, reduce.keep_a, reduce.send_b, reduce.keep_b, part_scr):
        ref[...] = jnp.zeros_like(ref)
    h_dec = (tok_ref[...].astype(F32) + a_ref[...].astype(F32)).astype(BF16)
    hd_ref[...] = h_dec.astype(F32)
    nd_ref[...] = rms(hd_ref[...], dg_ref[1:2, :])

    @pl.loop(0, steps)
    def _(i):
        j = i + F_SLOTS - 1

        @pl.when(j < steps)
        def _():
            for copy in loads(j, gup_hbm, dnp_hbm, lax.rem(j, F_SLOTS)):
                copy.start()

        @pl.when(j >= steps)
        def _():
            for copy in loads(j - steps, gud_hbm, dnd_hbm, lax.rem(j, F_SLOTS)):
                copy.start()

        slot = lax.rem(i, F_SLOTS)
        for copy in loads(i, gup_hbm, dnp_hbm, slot):
            copy.wait()
        product(i, slot, n_ref[...], lambda part, cols: reduce.put(part, cols, True))

    greeted(peers)
    for c in range(GROUPS):
        reduce.start(c)

    def add_dec(part, cols):
        c = cols.start // quarter
        part_scr[c, :, cols.start - c * quarter:cols.stop - c * quarter] += part

    def own_rows():
        for half, total in zip((0, 1), reduce.totals()):
            h = own_ref[half * piece:(half + 1) * piece, :].astype(F32)
            rows_all[0, half] = (h + total.astype(BF16).astype(F32)).astype(BF16)
        gather.start()

    @pl.loop(0, steps)
    def _(i):
        j = i + F_SLOTS - 1

        @pl.when(j < steps)
        def _():
            for copy in loads(j, gud_hbm, dnd_hbm, lax.rem(j + steps, F_SLOTS)):
                copy.start()

        slot = lax.rem(i + steps, F_SLOTS)
        for copy in loads(i, gud_hbm, dnd_hbm, slot):
            copy.wait()
        product(i, slot, nd_ref[...], add_dec)

        @pl.when(i == 2)
        def _():
            reduce.middle(0)

        @pl.when(i == 5)
        def _():
            reduce.middle(1)

        @pl.when(i == 8)
        def _():
            own_rows()

    for r in range(4):
        small.part[r] = part_scr[lax.bitwise_xor(y, r)]
    small.start()
    gather.forward()
    small.middle()
    small.finish(nd_ref)
    d_out[...] = (hd_ref[...] + nd_ref[...].astype(F32)).astype(BF16)
    reduce.drain()
    gather.finish()
    for r in range(4):
        owner = lax.bitwise_xor(y, r)
        for half in range(2):
            h_out[pl.ds(pl.multiple_of((2 * owner + half) * piece, piece), piece), :] = rows_all[r, half]


def cache_kernel(c_len, kt_ref, vt_ref, kc_hbm, vc_hbm, kn_hbm, vn_hbm, cache, in_sem, out_sem):
    batch = kt_ref.shape[0]

    def load(b, which):
        return pltpu.make_async_copy((kc_hbm, vc_hbm)[which].at[b], cache.at[which, b], in_sem.at[which, b])

    def store(b, which):
        return pltpu.make_async_copy(cache.at[which, b], (kn_hbm, vn_hbm)[which].at[b], out_sem.at[which, b])

    @pl.loop(0, batch)
    def _(b):
        load(b, 0).start()
        load(b, 1).start()

    @pl.loop(0, batch)
    def _(b):
        for which, tok in ((0, kt_ref), (1, vt_ref)):
            load(b, which).wait()
            cache[which, b, c_len[b]] = tok[b]
            store(b, which).start()

    @pl.loop(0, batch)
    def _(b):
        store(b, 0).wait()
        store(b, 1).wait()


def call(kernel, name, in_specs, out_specs, out_shape, scratch, us, collective_id=None):
    return pl.pallas_call(kernel, name=name, in_specs=in_specs, out_specs=out_specs, out_shape=out_shape, scratch_shapes=scratch,
                          cost_estimate=pl.CostEstimate(flops=int(us * 2e7), bytes_accessed=int(us * 3e6), transcendentals=0),
                          compiler_params=pltpu.CompilerParams(vmem_limit_bytes=62 * 2 ** 20, collective_id=collective_id, has_side_effects=collective_id is not None))


def shape(dims, dtype=F32):
    return jax.ShapeDtypeStruct(dims, dtype)


def solution(mesh):
    side = mesh.shape['side']
    inst_axes = ('pair', 'side')
    rows_spec = P(inst_axes, None)
    vec_spec = P(inst_axes)
    cache_spec = P(None, inst_axes, None, None, 'tp', None)
    prompt_spec = P(None, inst_axes, None, 'tp', None)
    in_specs = (rows_spec, vec_spec, P(None, None, None, 'tp', None), P(None, 'tp', None, None), P(None, None, 'tp', None), P(None, 'tp', None), P(None, None, None), rows_spec, cache_spec, cache_spec, vec_spec, P(None, None, None, None, 'tp', None), P(None, None, 'tp', None, None), P(None, None, 'tp', None), P(None, 'tp', None), P(None, None, None))
    out_specs = (rows_spec, rows_spec, prompt_spec, prompt_spec, cache_spec, cache_spec)

    def device_fn(prompt_x, s_len, w_qkv_pre, w_out_pre, w_gu_pre, w_down_pre, gain_pre, dec_tokens, k_cache, v_cache, c_len, w_qkv_dec, w_out_dec, w_gu_dec, w_down_dec, gain_dec):
        rows, width = prompt_x.shape
        batch = dec_tokens.shape[0]
        heads, head = w_qkv_pre.shape[3], w_qkv_pre.shape[4]
        cache_len = k_cache.shape[2]
        piece = rows // 8
        quarter = width // 4
        pairs = heads // 2
        dma = pltpu.SemaphoreType.DMA
        cos_tab, sin_tab = rope_rows(max(rows, cache_len), head)
        comm = RowReduce.scratch(piece, width) + RowGather.scratch(piece, width) + ColumnSum.scratch(batch, quarter)
        flat = (batch, cache_len * heads, head)
        wide = (batch, cache_len, heads, head)
        kv_block = pltpu.VMEM((4, 2, heads // 4, rows, head), BF16)
        h_own, n_all, a_all, k_tok, v_tok, k_prompt, v_prompt = call(
            functools.partial(attn_kernel, side), 'attn', [SMEM] * 2 + [VMEM] * 6 + [HBM] * 6, [VMEM] * 7,
            [shape((2 * piece, width), BF16), shape((4, 2, piece, width), BF16), shape((batch, width), BF16)] + [shape((batch, heads, head), BF16)] * 2 + [shape((rows, heads, head), BF16)] * 2,
            [pltpu.VMEM((D_SLOTS, D_BLOCK, 3, heads, head), BF16), dma((D_SLOTS,)), pltpu.VMEM((2, heads * head, width), BF16), dma((2,)),
             pltpu.VMEM((2,) + flat, BF16), dma((2, batch)),
             pltpu.VMEM((rows, width), BF16), pltpu.VMEM((3 * pairs, rows, 2 * head), F32), pltpu.VMEM((rows, heads * head), BF16), pltpu.VMEM((rows, heads * head), BF16),
             pltpu.VMEM((heads, rows, head), BF16), pltpu.VMEM((heads, rows, head), BF16),
             pltpu.VMEM((batch, width), BF16), pltpu.VMEM((3 * pairs, batch, 2 * head), F32), pltpu.VMEM((batch, heads, head), BF16), pltpu.VMEM((batch, heads, head), F32), pltpu.VMEM((4, batch, quarter), F32),
             kv_block, kv_block, dma((4,)), dma((4,))] + comm, 46, 0)(
            s_len, c_len, prompt_x, gain_pre[0], cos_tab, sin_tab, dec_tokens, gain_dec[0],
            w_qkv_pre[0], w_out_pre.reshape(heads * head, width), w_qkv_dec.reshape(width, 3, heads, head),
            k_cache.reshape(flat), v_cache.reshape(flat), w_out_dec.reshape(heads * head, width))
        h_out, dec_out = call(
            mlp_kernel, 'mlp', [VMEM] * 5 + [HBM] * 4, [VMEM] * 2, [shape((rows, width), BF16), shape((batch, width), BF16)],
            [pltpu.VMEM((F_SLOTS, F_BLOCK, width), BF16)] * 3 + [dma((3, F_SLOTS)), pltpu.VMEM((rows, width), BF16), pltpu.VMEM((batch, width), BF16), pltpu.VMEM((batch, width), F32), pltpu.VMEM((4, batch, quarter), F32)] + comm, 50, 1)(
            n_all, h_own, dec_tokens, a_all, gain_dec[0], w_gu_pre[0], w_down_pre[0], w_gu_dec[0], w_down_dec[0])
        k_new, v_new = call(
            cache_kernel, 'cache', [SMEM] + [VMEM] * 2 + [HBM] * 2, [HBM] * 2, [shape(wide, BF16)] * 2,
            [pltpu.VMEM((2,) + wide, BF16), dma((2, batch)), dma((2, batch))], 7)(c_len, k_tok, v_tok, k_cache.reshape(wide), v_cache.reshape(wide))
        prompt_shape = (1, rows, heads, 1, head)
        return h_out, dec_out, k_prompt.reshape(prompt_shape), v_prompt.reshape(prompt_shape), k_new.reshape(k_cache.shape), v_new.reshape(v_cache.shape)

    return jax.shard_map(device_fn, mesh=mesh, in_specs=in_specs, out_specs=out_specs, check_vma=False)
```

```python
import functools

import jax
import jax.numpy as jnp
import numpy as np
from jax import lax
from jax.experimental import pallas as pl
from jax.experimental.pallas import tpu as pltpu
from jax.sharding import PartitionSpec as P

EPSILON = 1e-6
THETA = 10000.0
MASKED = -1e30
D_BLOCK = 512
D_SLOTS = 3
F_BLOCK = 256
F_SLOTS = 4
LATE_SLOTS = 6
ROW_SLOTS = 4
N_BLOCK = 512
GROUPS = 2
F32 = jnp.float32
BF16 = jnp.bfloat16

MESH = pl.DeviceIdType.MESH

VMEM = pl.BlockSpec(memory_space=pltpu.VMEM)
SMEM = pl.BlockSpec(memory_space=pltpu.SMEM)
HBM = pl.BlockSpec(memory_space=pltpu.HBM)


def dot(lhs, rhs):
    return jnp.dot(lhs, rhs, preferred_element_type=F32)


def dot_nt(lhs, rhs):
    return lax.dot_general(lhs, rhs, (((1,), (1,)), ((), ())), preferred_element_type=F32)


def rms(values, gain):
    inv = lax.rsqrt(jnp.mean(values * values, axis=-1, keepdims=True) + EPSILON)
    return (values * inv * gain).astype(BF16)


def rope_rows(positions, head_dim):
    half = head_dim // 2
    inv_freq = np.power(np.float32(THETA), -np.arange(half, dtype=np.float32) * np.float32(2.0) / np.float32(head_dim)).astype(np.float32)
    angles = np.arange(positions, dtype=np.float32)[:, None] * inv_freq[None, :]
    cos_half = np.cos(angles).astype(np.float32)
    sin_half = np.sin(angles).astype(np.float32)
    return jnp.asarray(np.concatenate([cos_half, cos_half], 1)), jnp.asarray(np.concatenate([-sin_half, sin_half], 1))


def rotate(values, cos_b, sin_b):
    return values * cos_b + pltpu.roll(values, values.shape[-1] // 2, 1) * sin_b


def qkv_product(n_ref, block, at, acc):
    kinds, heads = block.shape[1], block.shape[2]
    nb = n_ref[:, pl.ds(pl.multiple_of(at * D_BLOCK, D_BLOCK), D_BLOCK)]
    for kind in range(kinds):
        by_head = jnp.swapaxes(block[:, kind], 0, 1)
        for p in range(heads // 2):
            pair = jnp.concatenate([by_head[2 * p], by_head[2 * p + 1]], axis=1)
            acc[kind * (heads // 2) + p] += dot(nb, pair)


def remote(src, dst, send_sem, recv_sem, where):
    return pltpu.make_async_remote_copy(src_ref=src, dst_ref=dst, send_sem=send_sem, recv_sem=recv_sem, device_id=where, device_id_type=MESH)


def greet(peers):
    barrier = pltpu.get_barrier_semaphore()
    for peer in peers:
        pl.semaphore_signal(barrier, inc=1, device_id=peer, device_id_type=MESH)


def greeted(peers):
    pl.semaphore_wait(pltpu.get_barrier_semaphore(), len(peers))


class RowReduce:
    def __init__(self, y, refs):
        (self.send_a, self.keep_a, self.send_b, self.keep_b, self.got_a, self.got_b,
         self.mid_a, self.mid_b, self.fin_a, self.fin_b, self.s_sem, self.r_sem) = refs
        self.near = {'tp': lax.bitwise_xor(y, 1)}
        self.wrap = {'tp': lax.bitwise_xor(y, 3)}

    @staticmethod
    def scratch(piece, width):
        part = width // GROUPS
        two, one = pltpu.VMEM((GROUPS, 2, piece, part), F32), pltpu.VMEM((GROUPS, piece, part), F32)
        return [two] * 6 + [one] * 4 + [pltpu.SemaphoreType.DMA((2, 2, GROUPS))] * 2

    def first(self, c):
        return (remote(self.send_a.at[c], self.got_a.at[c], self.s_sem.at[0, 0, c], self.r_sem.at[0, 0, c], self.near),
                remote(self.send_b.at[c], self.got_b.at[c], self.s_sem.at[0, 1, c], self.r_sem.at[0, 1, c], self.wrap))

    def second_of(self, i, c):
        mid, fin, where = ((self.mid_a, self.fin_a, self.wrap), (self.mid_b, self.fin_b, self.near))[i]
        return remote(mid.at[c], fin.at[c], self.s_sem.at[1, i, c], self.r_sem.at[1, i, c], where)

    def second(self, c):
        return self.second_of(0, c), self.second_of(1, c)

    def put(self, part, cols, add):
        q = part.shape[0] // 8
        piece = [part[i * q:(i + 1) * q] for i in range(8)]
        size = self.send_a.shape[-1]
        c = cols.start // size
        at = slice(cols.start - c * size, cols.stop - c * size)
        for ref, one, two in ((self.send_a, 2, 4), (self.keep_a, 0, 6), (self.send_b, 7, 5), (self.keep_b, 1, 3)):
            for row, i in ((0, one), (1, two)):
                ref[c, row, :, at] = ref[c, row, :, at] + piece[i] if add else piece[i]

    def start(self, c):
        for copy in self.first(c):
            copy.start()

    def middle(self, c):
        for copy, keep, got, mid, after in zip(self.first(c), (self.keep_a, self.keep_b), (self.got_a, self.got_b), (self.mid_a, self.mid_b), self.second(c)):
            copy.wait_recv()
            mid[c] = keep[c, 1] + got[c, 1]
            after.start()

    def totals(self, c):
        found = []
        for i, (keep, got, fin) in enumerate(((self.keep_a, self.got_a, self.fin_a), (self.keep_b, self.got_b, self.fin_b))):
            self.second_of(i, c).wait_recv()
            found.append((keep[c, 0] + got[c, 0]) + fin[c])
        return found

    def drain(self):
        for c in range(GROUPS):
            for copy in self.first(c) + self.second(c):
                copy.wait_send()


class RowGather:
    def __init__(self, y, rows, s_sem, r_sem):
        near, wrap = {'tp': lax.bitwise_xor(y, 1)}, {'tp': lax.bitwise_xor(y, 3)}
        moves = ((0, 0, 3, 0, wrap), (0, 1, 1, 1, near), (0, 0, 1, 0, near), (0, 1, 3, 1, wrap), (3, 0, 2, 0, near), (1, 1, 2, 1, wrap))
        part = rows.shape[-1] // GROUPS
        self.copies = []
        for c in range(GROUPS):
            at = pl.ds(c * part, part)
            self.copies.append([functools.partial(remote, rows.at[r, h, :, at], rows.at[to, h2, :, at], s_sem.at[c, i], r_sem.at[c, i], where) for i, (r, h, to, h2, where) in enumerate(moves)])

    @staticmethod
    def scratch(piece, width):
        return [pltpu.VMEM((4, 2, piece, width), BF16)] + [pltpu.SemaphoreType.DMA((GROUPS, 6))] * 2

    def start(self, c):
        for copy in self.copies[c][:4]:
            copy().start()

    def forward(self, c):
        for i in range(2):
            self.copies[c][i]().wait_recv()
            self.copies[c][4 + i]().start()

    def finish(self):
        for c in range(GROUPS):
            for copy in self.copies[c][2:]:
                copy().wait_recv()
            for copy in self.copies[c]:
                copy().wait_send()


class ColumnSum:
    def __init__(self, y, refs):
        self.y = y
        self.part, self.got, self.total, self.s_sem, self.r_sem = refs

    @staticmethod
    def scratch(batch, quarter):
        return [pltpu.VMEM((4, batch, quarter), F32), pltpu.VMEM((4, batch, quarter), F32), pltpu.VMEM((4, batch, quarter), BF16)] + [pltpu.SemaphoreType.DMA((2, 4))] * 2

    def copies(self, step):
        src, dst = ((self.part, self.got), (self.total, self.total))[step]
        return [remote(src.at[0 if step else r], dst.at[r], self.s_sem.at[step, r], self.r_sem.at[step, r], {'tp': lax.bitwise_xor(self.y, r)}) for r in (1, 2, 3)]

    def start(self):
        for copy in self.copies(0):
            copy.start()

    def middle(self):
        for copy in self.copies(0):
            copy.wait_recv()
        self.total[0] = ((self.part[0] + self.got[1]) + (self.got[2] + self.got[3])).astype(BF16)
        for copy in self.copies(1):
            copy.start()

    def finish(self, out_ref):
        for copy in self.copies(1):
            copy.wait_recv()
        quarter = self.total.shape[-1]
        for r in range(4):
            owner = lax.bitwise_xor(self.y, r)
            out_ref[:, pl.ds(pl.multiple_of(owner * quarter, quarter), quarter)] = self.total[r].astype(out_ref.dtype)
        for step in range(2):
            for copy in self.copies(step):
                copy.wait_send()


def layer_kernel(side, s_len, c_len, g_ref, cos_ref, sin_ref, tok_ref, dg_ref, x_hbm, wp_hbm, wop_hbm, wd_hbm, kc_hbm, vc_hbm, wod_hbm, gup_hbm, dnp_hbm, gud_hbm, dnd_hbm,
                 h_out, d_out, kt_ref, vt_ref, kp_ref, vp_ref,
                 x_ref, x_sem, buf, sem, ring, ring_sem, wo_sem, cache, cache_sem, n_ref, acc, ctx, ctx_rel, k_scr, v_scr, nd_ref, hd_ref, accd, q_scr, ctxd, part_scr, own_ref, m_ref, md_ref, late, late_sem,
                 kv_send, kv_got, kv_ssem, kv_rsem, *comm):
    y = lax.axis_index('tp')
    s = lax.axis_index('side')
    far = lax.rem(s + side // 2, side)
    near_peers = [{'tp': lax.bitwise_xor(y, r)} for r in (1, 2, 3)]
    far_peers = [{'tp': lax.bitwise_xor(y, r), 'side': far} for r in range(4)]
    reduce = RowReduce(y, comm[:12])
    rows_all = comm[12]
    gather = RowGather(y, *comm[12:15])
    small = ColumnSum(y, comm[15:20])
    rows, width = x_ref.shape
    batch = tok_ref.shape[0]
    heads, head = wp_hbm.shape[2], wp_hbm.shape[3]
    pairs = heads // 2
    steps = width // D_BLOCK
    ff = dnp_hbm.shape[0]
    f_steps = pl.cdiv(ff, F_BLOCK)
    wo_parts = heads * head // F_BLOCK
    scale = head ** -0.5
    group = width // GROUPS

    def load(i, w_hbm, slot):
        return pltpu.make_async_copy(w_hbm.at[pl.ds(i * D_BLOCK, D_BLOCK)], buf.at[slot], sem.at[slot])

    def wo_load(which):
        return pltpu.make_async_copy((wop_hbm, wod_hbm)[which], ring.at[pl.ds(which * wo_parts, wo_parts)], wo_sem.at[which])

    def f_at(i):
        return pl.multiple_of(jnp.minimum(i * F_BLOCK, ff - F_BLOCK), 8)

    def f_slot(i):
        return lax.rem(i + F_SLOTS - 1, F_SLOTS)

    def gu_loads(t, gu_hbm, i):
        at, slot = pl.ds(f_at(i), F_BLOCK), f_slot(t)
        return [pltpu.make_async_copy(gu_hbm.at[which, at], ring.at[3 * slot + which], ring_sem.at[which, slot]) for which in range(2)]

    def down_load(t, down_hbm, i, size):
        slot = f_slot(t)
        return pltpu.make_async_copy(down_hbm.at[pl.ds(f_at(i), F_BLOCK), pl.ds(0, size)], ring.at[3 * slot + 2, :, pl.ds(0, size)], ring_sem.at[2, slot])

    def f_start(t):
        @pl.when(t < f_steps)
        def _():
            for copy in gu_loads(t, gup_hbm, t):
                copy.start()

        @pl.when((t >= f_steps) & (t < 2 * f_steps))
        def _():
            for copy in gu_loads(t, gud_hbm, t - f_steps):
                copy.start()

        @pl.when((t > 0) & (t <= f_steps))
        def _():
            down_load(t, dnp_hbm, t - 1, group).start()

        @pl.when((t > f_steps) & (t <= 2 * f_steps))
        def _():
            down_load(t, dnd_hbm, t - 1 - f_steps, width).start()

    def cache_load(b, which):
        slot = lax.rem(b, ROW_SLOTS)
        return pltpu.make_async_copy((kc_hbm, vc_hbm)[which].at[b], cache.at[which, slot], cache_sem.at[which, slot])

    def late_load(i):
        slot = lax.rem(i, LATE_SLOTS)
        return pltpu.make_async_copy(dnp_hbm.at[pl.ds(f_at(i), F_BLOCK), pl.ds(group, group)], late.at[slot], late_sem.at[slot])

    x_copy = pltpu.make_async_copy(x_hbm, x_ref, x_sem)
    x_copy.start()
    load(0, wp_hbm, 0).start()
    greet(near_peers + far_peers)
    acc[...] = jnp.zeros_like(acc)
    accd[...] = jnp.zeros_like(accd)
    x_copy.wait()
    for i in range(1, D_SLOTS - 1):
        load(i, wp_hbm, i).start()

    @pl.loop(0, rows // 16)
    def _(i):
        r = pl.ds(pl.multiple_of(i * 16, 16), 16)
        n_ref[r, :] = rms(x_ref[r, :].astype(F32), g_ref[0:1, :])

    @pl.loop(0, steps)
    def _(i):
        j = i + D_SLOTS - 1

        @pl.when(j < steps)
        def _():
            load(j, wp_hbm, lax.rem(j, D_SLOTS)).start()

        @pl.when(j >= steps)
        def _():
            load(j - steps, wd_hbm, lax.rem(j, D_SLOTS)).start()

        @pl.when(i == 1)
        def _():
            wo_load(0).start()

        @pl.when(i == 3)
        def _():
            wo_load(1).start()

        @pl.when(i == 5)
        def _():
            f_start(0)

        slot = lax.rem(i, D_SLOTS)
        load(i, wp_hbm, slot).wait()
        qkv_product(n_ref, buf.at[slot], i, acc)

    @pl.loop(0, ROW_SLOTS)
    def _(b):
        cache_load(b, 0).start()
        cache_load(b, 1).start()

    cos_b, sin_b = cos_ref[:rows, :], sin_ref[:rows, :]
    row_id = lax.broadcasted_iota(jnp.int32, (rows, rows), 0)
    col_id = lax.broadcasted_iota(jnp.int32, (rows, rows), 1)
    allowed = (col_id <= row_id) & (col_id < s_len[0])

    @pl.loop(0, pairs)
    def _(p):
        pair_ctx = []
        for half in range(2):
            lanes = slice(half * head, (half + 1) * head)
            q = rotate(acc[p, :, lanes], cos_b, sin_b).astype(BF16)
            k = rotate(acc[pairs + p, :, lanes], cos_b, sin_b).astype(BF16)
            v = acc[2 * pairs + p, :, lanes].astype(BF16)
            k_scr[2 * p + half] = k
            v_scr[2 * p + half] = v
            scores = jnp.where(allowed, dot_nt(q, k) * scale, MASKED)
            top = jnp.max(scores, axis=-1, keepdims=True)
            weights = jnp.exp(scores - top)
            prob = (weights / jnp.sum(weights, axis=-1, keepdims=True)).astype(BF16)
            pair_ctx.append(dot(prob, v).astype(BF16))
        ctx[:, pl.ds(pl.multiple_of(p * 2 * head, 2 * head), 2 * head)] = jnp.concatenate(pair_ctx, axis=1)

    greeted(near_peers + far_peers)
    block = rows // 4
    for r in range(4):
        owner = lax.bitwise_xor(y, r)
        ctx_rel[r * block:(r + 1) * block, :] = ctx[pl.ds(pl.multiple_of(owner * block, block), block), :]
        for jj in range(heads // 4):
            kv_send[r, 0, jj] = k_scr[jj * 4 + owner]
            kv_send[r, 1, jj] = v_scr[jj * 4 + owner]
    kv_copies = [remote(kv_send.at[r], kv_got.at[r], kv_ssem.at[r], kv_rsem.at[r], far_peers[r]) for r in range(4)]
    wo_load(0).wait()

    def wo_product(lhs, which, cols):
        found = None
        for i in range(wo_parts):
            part = dot(lhs[:, i * F_BLOCK:(i + 1) * F_BLOCK], ring[which * wo_parts + i, :, cols])
            found = part if found is None else found + part
        return found

    lhs = ctx_rel[...]
    for c in range(width // N_BLOCK):
        cols = slice(c * N_BLOCK, (c + 1) * N_BLOCK)
        reduce.put(wo_product(lhs, 0, cols), cols, False)
        if cols.stop % group == 0:
            reduce.start(cols.start // group)
    f_start(1)
    nd_ref[...] = rms(tok_ref[...].astype(F32), dg_ref[0:1, :])

    @pl.loop(0, steps)
    def _(i):
        j = i + D_SLOTS - 1

        @pl.when(j < steps)
        def _():
            load(j, wd_hbm, lax.rem(j + steps, D_SLOTS)).start()

        slot = lax.rem(i + steps, D_SLOTS)
        load(i, wd_hbm, slot).wait()
        qkv_product(nd_ref, buf.at[slot], i, accd)

        @pl.when(i == 5)
        def _():
            reduce.middle(0)

    cos_d = jnp.concatenate([cos_ref[pl.ds(c_len[b], 1), :] for b in range(batch)], axis=0)
    sin_d = jnp.concatenate([sin_ref[pl.ds(c_len[b], 1), :] for b in range(batch)], axis=0)

    def by_row(kind, turn):
        found = []
        for h in range(heads):
            vals = accd[kind * pairs + h // 2, :, (h % 2) * head:(h % 2 + 1) * head]
            found.append(rotate(vals, cos_d, sin_d) if turn else vals)
        return jnp.swapaxes(jnp.stack(found), 0, 1).astype(BF16)

    q_scr[...] = by_row(0, True)
    kt_ref[...] = by_row(1, True)
    vt_ref[...] = by_row(2, False)
    slots = cache.shape[2]
    lane = lax.broadcasted_iota(jnp.int32, (heads, slots), 1)
    mine = lax.bitwise_and(lane, heads - 1) == lax.broadcasted_iota(jnp.int32, (heads, slots), 0)

    @pl.loop(0, batch)
    def _(b):
        @pl.when(b == 4)
        def _():
            reduce.middle(1)

        cache_load(b, 0).wait()
        cache_load(b, 1).wait()
        q, k_tok, v_tok = q_scr[b], kt_ref[b].astype(F32), vt_ref[b].astype(F32)
        row = lax.rem(b, ROW_SLOTS)
        scores = dot_nt(q, cache[0, row]) * scale
        scores = jnp.where(mine & (lane < c_len[b] * heads), scores, MASKED)
        own = jnp.sum(q.astype(F32) * k_tok, axis=-1, keepdims=True) * scale
        top = jnp.maximum(jnp.max(scores, axis=-1, keepdims=True), own)
        weights = jnp.exp(scores - top)
        own_w = jnp.exp(own - top)
        total = jnp.sum(weights, axis=-1, keepdims=True) + own_w
        prob = (weights / total).astype(BF16)
        own_prob = (own_w / total).astype(BF16).astype(F32)
        ctxd[b] = (dot(prob, cache[1, row]) + own_prob * v_tok).astype(BF16).astype(F32)

        @pl.when(b + ROW_SLOTS < batch)
        def _():
            cache_load(b + ROW_SLOTS, 0).start()
            cache_load(b + ROW_SLOTS, 1).start()

    by_head = jnp.swapaxes(ctxd[...], 0, 1)
    lhs_d = jnp.concatenate([by_head[h] for h in range(heads)], axis=1).astype(BF16)
    wo_load(1).wait()
    quarter = width // 4
    for c in range(4):
        part_scr[c] = wo_product(lhs_d, 1, slice(c * quarter, (c + 1) * quarter))
    for r in range(4):
        small.part[r] = part_scr[lax.bitwise_xor(y, r)]
    small.start()
    f_start(2)
    f_start(3)
    for i in range(LATE_SLOTS):
        late_load(i).start()

    piece = block // 2
    parts = [reduce.totals(c) for c in range(GROUPS)]
    for at in range(2):
        total = jnp.concatenate([part[at] for part in parts], axis=1)
        x_rows = x_ref[pl.ds(pl.multiple_of(y * block + at * piece, piece), piece), :]
        h = (x_rows.astype(F32) + total.astype(BF16).astype(F32)).astype(BF16)
        own_ref[at * piece:(at + 1) * piece, :] = h
        rows_all[0, at] = rms(h.astype(F32), g_ref[1:2, :])
    for c in range(GROUPS):
        gather.start(c)
    small.middle()
    for c in range(GROUPS):
        gather.forward(c)
    small.finish(nd_ref)
    h_dec = (tok_ref[...].astype(F32) + nd_ref[...].astype(F32)).astype(BF16)
    hd_ref[...] = h_dec.astype(F32)
    nd_ref[...] = rms(hd_ref[...], dg_ref[1:2, :])
    part_scr[...] = jnp.zeros_like(part_scr)
    reduce.drain()
    for ref in (reduce.send_a, reduce.keep_a, reduce.send_b, reduce.keep_b):
        ref[...] = jnp.zeros_like(ref)
    gather.finish()
    for copy in kv_copies:
        copy.start()
    for r in range(4):
        for half in range(2):
            i = (2 * r + half) * piece
            n_ref[i:i + piece, :] = rows_all[r, half]

    def gate_up(i, slot, n):
        tall = n.shape[0] >= 128
        gate, up = [(dot_nt(w, n) if tall else dot_nt(n, w)).astype(BF16).astype(F32) for w in (ring[3 * slot], ring[3 * slot + 1])]
        m = jax.nn.silu(gate) * up
        m = m.T if tall else m
        lane = lax.broadcasted_iota(jnp.int32, m.shape, 1)
        return jnp.where(f_at(i) + lane >= i * F_BLOCK, m, 0.0).astype(BF16)

    def down(m, slot, size, add):
        for c in range(size // N_BLOCK):
            cols = slice(c * N_BLOCK, (c + 1) * N_BLOCK)
            add(dot(m, ring[3 * slot + 2, :, cols]), cols)

    def stream_mlp(base, gu_hbm, down_hbm, size, n_rows, m_ref, add, beside):
        for copy in gu_loads(base, gu_hbm, 0):
            copy.wait()
        m_ref[0] = gate_up(0, f_slot(base), n_rows[...])

        @pl.loop(1, f_steps)
        def _(i):
            t = base + i
            f_start(t + F_SLOTS - 1)
            slot = f_slot(t)
            for copy in gu_loads(t, gu_hbm, i):
                copy.wait()
            down_load(t, down_hbm, i - 1, size).wait()
            before = m_ref[i - 1]
            after = gate_up(i, slot, n_rows[...])
            down(before, slot, size, add)
            m_ref[i] = after
            beside(i)

        t = base + f_steps
        f_start(t + F_SLOTS - 1)
        down_load(t, down_hbm, f_steps - 1, size).wait()
        down(m_ref[f_steps - 1], f_slot(t), size, add)

    def add_pre(part, cols):
        reduce.put(part, cols, True)

    stream_mlp(0, gup_hbm, dnp_hbm, group, n_ref, m_ref, add_pre, lambda i: None)
    reduce.start(0)

    @pl.loop(0, f_steps)
    def _(i):
        late_load(i).wait()
        m = m_ref[i]
        for c in range(group // N_BLOCK):
            at = c * N_BLOCK
            add_pre(dot(m, late[lax.rem(i, LATE_SLOTS), :, at:at + N_BLOCK]), slice(group + at, group + at + N_BLOCK))

        @pl.when(i + LATE_SLOTS < f_steps)
        def _():
            late_load(i + LATE_SLOTS).start()

    reduce.start(1)

    def add_dec(part, cols):
        c = cols.start // quarter
        part_scr[c, :, cols.start - c * quarter:cols.stop - c * quarter] += part

    def own_rows(c):
        cols = slice(c * group, (c + 1) * group)
        for half, total in zip((0, 1), reduce.totals(c)):
            h = own_ref[half * piece:(half + 1) * piece, cols].astype(F32)
            rows_all[0, half, :, cols] = (h + total.astype(BF16).astype(F32)).astype(BF16)
        gather.start(c)

    def between(i):
        @pl.when(i == 1)
        def _():
            reduce.middle(0)

        @pl.when(i == 5)
        def _():
            reduce.middle(1)

        @pl.when(i == 6)
        def _():
            own_rows(0)

        @pl.when(i == 8)
        def _():
            gather.forward(0)

        @pl.when(i == 9)
        def _():
            own_rows(1)

    stream_mlp(f_steps, gud_hbm, dnd_hbm, width, nd_ref, md_ref, add_dec, between)
    for r in range(4):
        small.part[r] = part_scr[lax.bitwise_xor(y, r)]
    small.start()
    gather.forward(1)
    small.middle()
    for r in range(4):
        kv_copies[r].wait_recv()
        owner = lax.bitwise_xor(y, r)
        for jj in range(heads // 4):
            k_scr[owner * (heads // 4) + jj] = kv_got[r, 0, jj]
            v_scr[owner * (heads // 4) + jj] = kv_got[r, 1, jj]
    kp_ref[...] = jnp.swapaxes(k_scr[...], 0, 1)
    vp_ref[...] = jnp.swapaxes(v_scr[...], 0, 1)
    small.finish(nd_ref)
    d_out[...] = (hd_ref[...] + nd_ref[...].astype(F32)).astype(BF16)
    reduce.drain()
    for copy in kv_copies:
        copy.wait_send()
    gather.finish()
    for r in range(4):
        owner = lax.bitwise_xor(y, r)
        for half in range(2):
            h_out[pl.ds(pl.multiple_of((2 * owner + half) * piece, piece), piece), :] = rows_all[r, half]


def finish_kernel(c_len, kt_ref, vt_ref, kc_hbm, vc_hbm, h_in, d_in, kp_in, vp_in, kn_hbm, vn_hbm, h_hbm, d_hbm, kp_hbm, vp_hbm, cache, h_buf, d_buf, kp_buf, vp_buf, in_sem, out_sem, m_in, m_out):
    batch = kt_ref.shape[0]
    moved = ((h_in, h_buf, h_hbm), (d_in, d_buf, d_hbm), (kp_in, kp_buf, kp_hbm), (vp_in, vp_buf, vp_hbm))

    def load(b, which):
        return pltpu.make_async_copy((kc_hbm, vc_hbm)[which].at[b], cache.at[which, b], in_sem.at[which, b])

    def store(b, which):
        return pltpu.make_async_copy(cache.at[which, b], (kn_hbm, vn_hbm)[which].at[b], out_sem.at[which, b])

    @pl.loop(0, batch)
    def _(b):
        load(b, 0).start()
        load(b, 1).start()

    ins = [pltpu.make_async_copy(src, mid, m_in.at[i]) for i, (src, mid, _) in enumerate(moved)]
    outs = [pltpu.make_async_copy(mid, dst, m_out.at[i]) for i, (_, mid, dst) in enumerate(moved)]
    for copy in ins:
        copy.start()

    @pl.loop(0, batch)
    def _(b):
        for which, tok in ((0, kt_ref), (1, vt_ref)):
            load(b, which).wait()
            cache[which, b, c_len[b]] = tok[b]
            store(b, which).start()

    for first, second in zip(ins, outs):
        first.wait()
        second.start()

    @pl.loop(0, batch)
    def _(b):
        store(b, 0).wait()
        store(b, 1).wait()

    for copy in outs:
        copy.wait()


def call(kernel, name, in_specs, out_specs, out_shape, scratch, us, collective_id=None):
    return pl.pallas_call(kernel, name=name, in_specs=in_specs, out_specs=out_specs, out_shape=out_shape, scratch_shapes=scratch,
                          cost_estimate=pl.CostEstimate(flops=int(us * 2e7), bytes_accessed=int(us * 3e6), transcendentals=0),
                          compiler_params=pltpu.CompilerParams(vmem_limit_bytes=62 * 2 ** 20, collective_id=collective_id, has_side_effects=collective_id is not None))


def shape(dims, dtype=F32):
    return jax.ShapeDtypeStruct(dims, dtype)


def solution(mesh):
    side = mesh.shape['side']
    inst_axes = ('pair', 'side')
    rows_spec = P(inst_axes, None)
    vec_spec = P(inst_axes)
    cache_spec = P(None, inst_axes, None, None, 'tp', None)
    prompt_spec = P(None, inst_axes, None, 'tp', None)
    in_specs = (rows_spec, vec_spec, P(None, None, None, 'tp', None), P(None, 'tp', None, None), P(None, None, 'tp', None), P(None, 'tp', None), P(None, None, None), rows_spec, cache_spec, cache_spec, vec_spec, P(None, None, None, None, 'tp', None), P(None, None, 'tp', None, None), P(None, None, 'tp', None), P(None, 'tp', None), P(None, None, None))
    out_specs = (rows_spec, rows_spec, prompt_spec, prompt_spec, cache_spec, cache_spec)

    def device_fn(prompt_x, s_len, w_qkv_pre, w_out_pre, w_gu_pre, w_down_pre, gain_pre, dec_tokens, k_cache, v_cache, c_len, w_qkv_dec, w_out_dec, w_gu_dec, w_down_dec, gain_dec):
        rows, width = prompt_x.shape
        batch = dec_tokens.shape[0]
        heads, head = w_qkv_pre.shape[3], w_qkv_pre.shape[4]
        cache_len = k_cache.shape[2]
        piece = rows // 8
        quarter = width // 4
        pairs = heads // 2
        f_steps = pl.cdiv(w_down_pre.shape[1], F_BLOCK)
        dma = pltpu.SemaphoreType.DMA
        cos_tab, sin_tab = rope_rows(max(rows, cache_len), head)
        comm = RowReduce.scratch(piece, width) + RowGather.scratch(piece, width) + ColumnSum.scratch(batch, quarter)
        flat = (batch, cache_len * heads, head)
        wide = (batch, cache_len, heads, head)
        kv_block = pltpu.VMEM((4, 2, heads // 4, rows, head), BF16)
        rows_shape, tok_shape, kv_shape, out_shape = shape((rows, width), BF16), shape((batch, heads, head), BF16), shape((rows, heads, head), BF16), shape((batch, width), BF16)
        h_out, dec_out, k_tok, v_tok, k_prompt, v_prompt = call(
            functools.partial(layer_kernel, side), 'layer', [SMEM] * 2 + [VMEM] * 5 + [HBM] * 11, [VMEM] * 6,
            [rows_shape, out_shape, tok_shape, tok_shape, kv_shape, kv_shape],
            [pltpu.VMEM((rows, width), BF16), dma, pltpu.VMEM((D_SLOTS, D_BLOCK, 3, heads, head), BF16), dma((D_SLOTS,)),
             pltpu.VMEM((3 * F_SLOTS, F_BLOCK, width), BF16), dma((3, F_SLOTS)), dma((2,)), pltpu.VMEM((2, ROW_SLOTS) + flat[1:], BF16), dma((2, ROW_SLOTS)),
             pltpu.VMEM((rows, width), BF16), pltpu.VMEM((3 * pairs, rows, 2 * head), F32), pltpu.VMEM((rows, heads * head), BF16), pltpu.VMEM((rows, heads * head), BF16),
             pltpu.VMEM((heads, rows, head), BF16), pltpu.VMEM((heads, rows, head), BF16),
             pltpu.VMEM((batch, width), BF16), pltpu.VMEM((batch, width), F32), pltpu.VMEM((3 * pairs, batch, 2 * head), F32), pltpu.VMEM((batch, heads, head), BF16), pltpu.VMEM((batch, heads, head), F32), pltpu.VMEM((4, batch, quarter), F32),
              pltpu.VMEM((2 * piece, width), BF16), pltpu.VMEM((f_steps, rows, F_BLOCK), BF16), pltpu.VMEM((f_steps, batch, F_BLOCK), BF16), pltpu.VMEM((LATE_SLOTS, F_BLOCK, width // GROUPS), BF16), dma((LATE_SLOTS,)), kv_block, kv_block, dma((4,)), dma((4,))] + comm, 90, 0)(
            s_len, c_len, gain_pre[0], cos_tab, sin_tab, dec_tokens, gain_dec[0], prompt_x,
            w_qkv_pre[0], w_out_pre.reshape(heads * head // F_BLOCK, F_BLOCK, width), w_qkv_dec.reshape(width, 3, heads, head),
            k_cache.reshape(flat), v_cache.reshape(flat), w_out_dec.reshape(heads * head // F_BLOCK, F_BLOCK, width),
            w_gu_pre[0], w_down_pre[0], w_gu_dec[0], w_down_dec[0])
        k_new, v_new, h_out, dec_out, k_prompt, v_prompt = call(
            finish_kernel, 'finish', [SMEM] + [VMEM] * 2 + [HBM] * 6, [HBM] * 6, [shape(wide, BF16)] * 2 + [rows_shape, out_shape, kv_shape, kv_shape],
            [pltpu.VMEM((2,) + wide, BF16), pltpu.VMEM((rows, width), BF16), pltpu.VMEM((batch, width), BF16), pltpu.VMEM((rows, heads, head), BF16), pltpu.VMEM((rows, heads, head), BF16),
             dma((2, batch)), dma((2, batch)), dma((4,)), dma((4,))], 7)(
            c_len, k_tok, v_tok, k_cache.reshape(wide), v_cache.reshape(wide), h_out, dec_out, k_prompt, v_prompt)
        prompt_shape = (1, rows, heads, 1, head)
        return h_out, dec_out, k_prompt.reshape(prompt_shape), v_prompt.reshape(prompt_shape), k_new.reshape(k_cache.shape), v_new.reshape(v_cache.shape)

    return jax.shard_map(device_fn, mesh=mesh, in_specs=in_specs, out_specs=out_specs, check_vma=False)
```

```python
import functools

import jax
import jax.numpy as jnp
import numpy as np
from jax import lax
from jax.experimental import pallas as pl
from jax.experimental.pallas import tpu as pltpu
from jax.sharding import PartitionSpec as P

EPSILON = 1e-6
THETA = 10000.0
MASKED = -1e30
D_BLOCK = 512
D_SLOTS = 3
F_BLOCK = 256
F_SLOTS = 4
LATE_SLOTS = 6
ROW_SLOTS = 4
N_BLOCK = 512
GROUPS = 2
F32 = jnp.float32
BF16 = jnp.bfloat16

MESH = pl.DeviceIdType.MESH

VMEM = pl.BlockSpec(memory_space=pltpu.VMEM)
SMEM = pl.BlockSpec(memory_space=pltpu.SMEM)
HBM = pl.BlockSpec(memory_space=pltpu.HBM)


def dot(lhs, rhs):
    return jnp.dot(lhs, rhs, preferred_element_type=F32)


def dot_nt(lhs, rhs):
    return lax.dot_general(lhs, rhs, (((1,), (1,)), ((), ())), preferred_element_type=F32)


def rms(values, gain):
    inv = lax.rsqrt(jnp.mean(values * values, axis=-1, keepdims=True) + EPSILON)
    return (values * inv * gain).astype(BF16)


def rope_rows(positions, head_dim):
    half = head_dim // 2
    inv_freq = np.power(np.float32(THETA), -np.arange(half, dtype=np.float32) * np.float32(2.0) / np.float32(head_dim)).astype(np.float32)
    angles = np.arange(positions, dtype=np.float32)[:, None] * inv_freq[None, :]
    cos_half = np.cos(angles).astype(np.float32)
    sin_half = np.sin(angles).astype(np.float32)
    return jnp.asarray(np.concatenate([cos_half, cos_half], 1)), jnp.asarray(np.concatenate([-sin_half, sin_half], 1))


def rotate(values, cos_b, sin_b):
    return values * cos_b + pltpu.roll(values, values.shape[-1] // 2, 1) * sin_b


def qkv_product(n_ref, block, at, acc):
    kinds, heads = block.shape[1], block.shape[2]
    nb = n_ref[:, pl.ds(pl.multiple_of(at * D_BLOCK, D_BLOCK), D_BLOCK)]
    for kind in range(kinds):
        by_head = jnp.swapaxes(block[:, kind], 0, 1)
        for p in range(heads // 2):
            pair = jnp.concatenate([by_head[2 * p], by_head[2 * p + 1]], axis=1)
            acc[kind * (heads // 2) + p] += dot(nb, pair)


def remote(src, dst, send_sem, recv_sem, where):
    return pltpu.make_async_remote_copy(src_ref=src, dst_ref=dst, send_sem=send_sem, recv_sem=recv_sem, device_id=where, device_id_type=MESH)


def greet(peers):
    barrier = pltpu.get_barrier_semaphore()
    for peer in peers:
        pl.semaphore_signal(barrier, inc=1, device_id=peer, device_id_type=MESH)


def greeted(peers):
    pl.semaphore_wait(pltpu.get_barrier_semaphore(), len(peers))


class RowReduce:
    def __init__(self, y, refs):
        (self.send_a, self.keep_a, self.send_b, self.keep_b, self.got_a, self.got_b,
         self.mid_a, self.mid_b, self.fin_a, self.fin_b, self.s_sem, self.r_sem) = refs
        self.near = {'tp': lax.bitwise_xor(y, 1)}
        self.wrap = {'tp': lax.bitwise_xor(y, 3)}

    @staticmethod
    def scratch(piece, width):
        part = width // GROUPS
        two, one = pltpu.VMEM((GROUPS, 2, piece, part), F32), pltpu.VMEM((GROUPS, piece, part), F32)
        return [two] * 6 + [one] * 4 + [pltpu.SemaphoreType.DMA((2, 2, GROUPS))] * 2

    def first(self, c):
        return (remote(self.send_a.at[c], self.got_a.at[c], self.s_sem.at[0, 0, c], self.r_sem.at[0, 0, c], self.near),
                remote(self.send_b.at[c], self.got_b.at[c], self.s_sem.at[0, 1, c], self.r_sem.at[0, 1, c], self.wrap))

    def second_of(self, i, c):
        mid, fin, where = ((self.mid_a, self.fin_a, self.wrap), (self.mid_b, self.fin_b, self.near))[i]
        return remote(mid.at[c], fin.at[c], self.s_sem.at[1, i, c], self.r_sem.at[1, i, c], where)

    def second(self, c):
        return self.second_of(0, c), self.second_of(1, c)

    def put(self, part, cols, add):
        q = part.shape[0] // 8
        piece = [part[i * q:(i + 1) * q] for i in range(8)]
        size = self.send_a.shape[-1]
        c = cols.start // size
        at = slice(cols.start - c * size, cols.stop - c * size)
        for ref, one, two in ((self.send_a, 2, 4), (self.keep_a, 0, 6), (self.send_b, 7, 5), (self.keep_b, 1, 3)):
            for row, i in ((0, one), (1, two)):
                ref[c, row, :, at] = ref[c, row, :, at] + piece[i] if add else piece[i]

    def start(self, c):
        for copy in self.first(c):
            copy.start()

    def middle(self, c):
        for copy, keep, got, mid, after in zip(self.first(c), (self.keep_a, self.keep_b), (self.got_a, self.got_b), (self.mid_a, self.mid_b), self.second(c)):
            copy.wait_recv()
            mid[c] = keep[c, 1] + got[c, 1]
            after.start()

    def totals(self, c):
        found = []
        for i, (keep, got, fin) in enumerate(((self.keep_a, self.got_a, self.fin_a), (self.keep_b, self.got_b, self.fin_b))):
            self.second_of(i, c).wait_recv()
            found.append((keep[c, 0] + got[c, 0]) + fin[c])
        return found

    def drain(self):
        for c in range(GROUPS):
            for copy in self.first(c) + self.second(c):
                copy.wait_send()


class RowGather:
    def __init__(self, y, rows, s_sem, r_sem):
        near, wrap = {'tp': lax.bitwise_xor(y, 1)}, {'tp': lax.bitwise_xor(y, 3)}
        moves = ((0, 0, 3, 0, wrap), (0, 1, 1, 1, near), (0, 0, 1, 0, near), (0, 1, 3, 1, wrap), (3, 0, 2, 0, near), (1, 1, 2, 1, wrap))
        part = rows.shape[-1] // GROUPS
        self.copies = []
        for c in range(GROUPS):
            at = pl.ds(c * part, part)
            self.copies.append([functools.partial(remote, rows.at[r, h, :, at], rows.at[to, h2, :, at], s_sem.at[c, i], r_sem.at[c, i], where) for i, (r, h, to, h2, where) in enumerate(moves)])

    @staticmethod
    def scratch(piece, width):
        return [pltpu.VMEM((4, 2, piece, width), BF16)] + [pltpu.SemaphoreType.DMA((GROUPS, 6))] * 2

    def start(self, c):
        for copy in self.copies[c][:4]:
            copy().start()

    def forward(self, c):
        for i in range(2):
            self.copies[c][i]().wait_recv()
            self.copies[c][4 + i]().start()

    def finish(self):
        for c in range(GROUPS):
            for copy in self.copies[c][2:]:
                copy().wait_recv()
            for copy in self.copies[c]:
                copy().wait_send()


class ColumnSum:
    def __init__(self, y, refs):
        self.y = y
        self.part, self.got, self.total, self.s_sem, self.r_sem = refs

    @staticmethod
    def scratch(batch, quarter):
        return [pltpu.VMEM((4, batch, quarter), F32), pltpu.VMEM((4, batch, quarter), F32), pltpu.VMEM((4, batch, quarter), BF16)] + [pltpu.SemaphoreType.DMA((2, 4))] * 2

    def copies(self, step):
        src, dst = ((self.part, self.got), (self.total, self.total))[step]
        return [remote(src.at[0 if step else r], dst.at[r], self.s_sem.at[step, r], self.r_sem.at[step, r], {'tp': lax.bitwise_xor(self.y, r)}) for r in (1, 2, 3)]

    def start(self):
        for copy in self.copies(0):
            copy.start()

    def middle(self):
        for copy in self.copies(0):
            copy.wait_recv()
        self.total[0] = ((self.part[0] + self.got[1]) + (self.got[2] + self.got[3])).astype(BF16)
        for copy in self.copies(1):
            copy.start()

    def finish(self, out_ref):
        for copy in self.copies(1):
            copy.wait_recv()
        quarter = self.total.shape[-1]
        for r in range(4):
            owner = lax.bitwise_xor(self.y, r)
            out_ref[:, pl.ds(pl.multiple_of(owner * quarter, quarter), quarter)] = self.total[r].astype(out_ref.dtype)
        for step in range(2):
            for copy in self.copies(step):
                copy.wait_send()


def layer_kernel(side, s_len, c_len, g_hbm, cos_hbm, sin_hbm, tok_hbm, dg_hbm, x_hbm, wp_hbm, wop_hbm, wd_hbm, kc_hbm, vc_hbm, wod_hbm, gup_hbm, dnp_hbm, gud_hbm, dnd_hbm,
                 h_out, d_out, kt_ref, vt_ref, kp_ref, vp_ref,
                 x_ref, g_ref, cos_ref, sin_ref, tok_ref, dg_ref, x_sem, buf, sem, ring, ring_sem, wo_sem, cache, cache_sem, n_ref, acc, ctx, ctx_rel, k_scr, v_scr, nd_ref, hd_ref, accd, q_scr, ctxd, part_scr, own_ref, m_ref, md_ref, late, late_sem,
                 kv_send, kv_got, kv_ssem, kv_rsem, *comm):
    y = lax.axis_index('tp')
    s = lax.axis_index('side')
    far = lax.rem(s + side // 2, side)
    near_peers = [{'tp': lax.bitwise_xor(y, r)} for r in (1, 2, 3)]
    far_peers = [{'tp': lax.bitwise_xor(y, r), 'side': far} for r in range(4)]
    reduce = RowReduce(y, comm[:12])
    rows_all = comm[12]
    gather = RowGather(y, *comm[12:15])
    small = ColumnSum(y, comm[15:20])
    rows, width = x_ref.shape
    batch = tok_ref.shape[0]
    heads, head = wp_hbm.shape[2], wp_hbm.shape[3]
    pairs = heads // 2
    steps = width // D_BLOCK
    ff = dnp_hbm.shape[0]
    f_steps = pl.cdiv(ff, F_BLOCK)
    wo_parts = heads * head // F_BLOCK
    scale = head ** -0.5
    group = width // GROUPS

    def load(i, w_hbm, slot):
        return pltpu.make_async_copy(w_hbm.at[pl.ds(i * D_BLOCK, D_BLOCK)], buf.at[slot], sem.at[slot])

    def wo_load(which):
        return pltpu.make_async_copy((wop_hbm, wod_hbm)[which], ring.at[pl.ds(which * wo_parts, wo_parts)], wo_sem.at[which])

    def f_at(i):
        return pl.multiple_of(jnp.minimum(i * F_BLOCK, ff - F_BLOCK), 8)

    def f_slot(i):
        return lax.rem(i + F_SLOTS - 1, F_SLOTS)

    def gu_loads(t, gu_hbm, i):
        at, slot = pl.ds(f_at(i), F_BLOCK), f_slot(t)
        return [pltpu.make_async_copy(gu_hbm.at[which, at], ring.at[3 * slot + which], ring_sem.at[which, slot]) for which in range(2)]

    def down_load(t, down_hbm, i, size):
        slot = f_slot(t)
        return pltpu.make_async_copy(down_hbm.at[pl.ds(f_at(i), F_BLOCK), pl.ds(0, size)], ring.at[3 * slot + 2, :, pl.ds(0, size)], ring_sem.at[2, slot])

    def f_start(t):
        @pl.when(t < f_steps)
        def _():
            for copy in gu_loads(t, gup_hbm, t):
                copy.start()

        @pl.when((t >= f_steps) & (t < 2 * f_steps))
        def _():
            for copy in gu_loads(t, gud_hbm, t - f_steps):
                copy.start()

        @pl.when((t > 0) & (t <= f_steps))
        def _():
            down_load(t, dnp_hbm, t - 1, group).start()

        @pl.when((t > f_steps) & (t <= 2 * f_steps))
        def _():
            down_load(t, dnd_hbm, t - 1 - f_steps, width).start()

    def cache_load(b, which):
        slot = lax.rem(b, ROW_SLOTS)
        return pltpu.make_async_copy((kc_hbm, vc_hbm)[which].at[b], cache.at[which, slot], cache_sem.at[which, slot])

    def late_load(i):
        slot = lax.rem(i, LATE_SLOTS)
        return pltpu.make_async_copy(dnp_hbm.at[pl.ds(f_at(i), F_BLOCK), pl.ds(group, group)], late.at[slot], late_sem.at[slot])

    smalls = [pltpu.make_async_copy(src, dst, x_sem.at[i]) for i, (src, dst) in enumerate(((x_hbm, x_ref), (g_hbm, g_ref), (cos_hbm, cos_ref), (sin_hbm, sin_ref), (tok_hbm, tok_ref), (dg_hbm, dg_ref)))]
    for copy in smalls:
        copy.start()
    load(0, wp_hbm, 0).start()
    greet(near_peers + far_peers)
    acc[...] = jnp.zeros_like(acc)
    accd[...] = jnp.zeros_like(accd)
    for copy in smalls:
        copy.wait()
    for i in range(1, D_SLOTS - 1):
        load(i, wp_hbm, i).start()

    @pl.loop(0, rows // 16)
    def _(i):
        r = pl.ds(pl.multiple_of(i * 16, 16), 16)
        n_ref[r, :] = rms(x_ref[r, :].astype(F32), g_ref[0:1, :])

    @pl.loop(0, steps)
    def _(i):
        j = i + D_SLOTS - 1

        @pl.when(j < steps)
        def _():
            load(j, wp_hbm, lax.rem(j, D_SLOTS)).start()

        @pl.when(j >= steps)
        def _():
            load(j - steps, wd_hbm, lax.rem(j, D_SLOTS)).start()

        @pl.when(i == 1)
        def _():
            wo_load(0).start()

        @pl.when(i == 3)
        def _():
            wo_load(1).start()

        @pl.when(i == 5)
        def _():
            f_start(0)

        slot = lax.rem(i, D_SLOTS)
        load(i, wp_hbm, slot).wait()
        qkv_product(n_ref, buf.at[slot], i, acc)

    @pl.loop(0, ROW_SLOTS)
    def _(b):
        cache_load(b, 0).start()
        cache_load(b, 1).start()

    cos_b, sin_b = cos_ref[:rows, :], sin_ref[:rows, :]
    row_id = lax.broadcasted_iota(jnp.int32, (rows, rows), 0)
    col_id = lax.broadcasted_iota(jnp.int32, (rows, rows), 1)
    allowed = (col_id <= row_id) & (col_id < s_len[0])

    @pl.loop(0, pairs)
    def _(p):
        pair_ctx = []
        for half in range(2):
            lanes = slice(half * head, (half + 1) * head)
            q = rotate(acc[p, :, lanes], cos_b, sin_b).astype(BF16)
            k = rotate(acc[pairs + p, :, lanes], cos_b, sin_b).astype(BF16)
            v = acc[2 * pairs + p, :, lanes].astype(BF16)
            k_scr[2 * p + half] = k
            v_scr[2 * p + half] = v
            scores = jnp.where(allowed, dot_nt(q, k) * scale, MASKED)
            top = jnp.max(scores, axis=-1, keepdims=True)
            weights = jnp.exp(scores - top)
            prob = (weights / jnp.sum(weights, axis=-1, keepdims=True)).astype(BF16)
            pair_ctx.append(dot(prob, v).astype(BF16))
        ctx[:, pl.ds(pl.multiple_of(p * 2 * head, 2 * head), 2 * head)] = jnp.concatenate(pair_ctx, axis=1)

    greeted(near_peers + far_peers)
    block = rows // 4
    for r in range(4):
        owner = lax.bitwise_xor(y, r)
        ctx_rel[r * block:(r + 1) * block, :] = ctx[pl.ds(pl.multiple_of(owner * block, block), block), :]
        for jj in range(heads // 4):
            kv_send[r, 0, jj] = k_scr[jj * 4 + owner]
            kv_send[r, 1, jj] = v_scr[jj * 4 + owner]
    kv_copies = [remote(kv_send.at[r], kv_got.at[r], kv_ssem.at[r], kv_rsem.at[r], far_peers[r]) for r in range(4)]
    wo_load(0).wait()

    def wo_product(lhs, which, cols):
        found = None
        for i in range(wo_parts):
            part = dot(lhs[:, i * F_BLOCK:(i + 1) * F_BLOCK], ring[which * wo_parts + i, :, cols])
            found = part if found is None else found + part
        return found

    lhs = ctx_rel[...]
    for c in range(width // N_BLOCK):
        cols = slice(c * N_BLOCK, (c + 1) * N_BLOCK)
        reduce.put(wo_product(lhs, 0, cols), cols, False)
        if cols.stop % group == 0:
            reduce.start(cols.start // group)
    f_start(1)
    nd_ref[...] = rms(tok_ref[...].astype(F32), dg_ref[0:1, :])

    @pl.loop(0, steps)
    def _(i):
        j = i + D_SLOTS - 1

        @pl.when(j < steps)
        def _():
            load(j, wd_hbm, lax.rem(j + steps, D_SLOTS)).start()

        slot = lax.rem(i + steps, D_SLOTS)
        load(i, wd_hbm, slot).wait()
        qkv_product(nd_ref, buf.at[slot], i, accd)

        @pl.when(i == 5)
        def _():
            reduce.middle(0)

    cos_d = jnp.concatenate([cos_ref[pl.ds(c_len[b], 1), :] for b in range(batch)], axis=0)
    sin_d = jnp.concatenate([sin_ref[pl.ds(c_len[b], 1), :] for b in range(batch)], axis=0)

    def by_row(kind, turn):
        found = []
        for h in range(heads):
            vals = accd[kind * pairs + h // 2, :, (h % 2) * head:(h % 2 + 1) * head]
            found.append(rotate(vals, cos_d, sin_d) if turn else vals)
        return jnp.swapaxes(jnp.stack(found), 0, 1).astype(BF16)

    q_scr[...] = by_row(0, True)
    kt_ref[...] = by_row(1, True)
    vt_ref[...] = by_row(2, False)
    slots = cache.shape[2]
    lane = lax.broadcasted_iota(jnp.int32, (heads, slots), 1)
    mine = lax.bitwise_and(lane, heads - 1) == lax.broadcasted_iota(jnp.int32, (heads, slots), 0)

    @pl.loop(0, batch)
    def _(b):
        @pl.when(b == 4)
        def _():
            reduce.middle(1)

        cache_load(b, 0).wait()
        cache_load(b, 1).wait()
        q, k_tok, v_tok = q_scr[b], kt_ref[b].astype(F32), vt_ref[b].astype(F32)
        row = lax.rem(b, ROW_SLOTS)
        scores = dot_nt(q, cache[0, row]) * scale
        scores = jnp.where(mine & (lane < c_len[b] * heads), scores, MASKED)
        own = jnp.sum(q.astype(F32) * k_tok, axis=-1, keepdims=True) * scale
        top = jnp.maximum(jnp.max(scores, axis=-1, keepdims=True), own)
        weights = jnp.exp(scores - top)
        own_w = jnp.exp(own - top)
        total = jnp.sum(weights, axis=-1, keepdims=True) + own_w
        prob = (weights / total).astype(BF16)
        own_prob = (own_w / total).astype(BF16).astype(F32)
        ctxd[b] = (dot(prob, cache[1, row]) + own_prob * v_tok).astype(BF16).astype(F32)

        @pl.when(b + ROW_SLOTS < batch)
        def _():
            cache_load(b + ROW_SLOTS, 0).start()
            cache_load(b + ROW_SLOTS, 1).start()

    by_head = jnp.swapaxes(ctxd[...], 0, 1)
    lhs_d = jnp.concatenate([by_head[h] for h in range(heads)], axis=1).astype(BF16)
    wo_load(1).wait()
    quarter = width // 4
    for c in range(4):
        part_scr[c] = wo_product(lhs_d, 1, slice(c * quarter, (c + 1) * quarter))
    for r in range(4):
        small.part[r] = part_scr[lax.bitwise_xor(y, r)]
    small.start()
    f_start(2)
    f_start(3)
    for i in range(LATE_SLOTS):
        late_load(i).start()

    piece = block // 2
    parts = [reduce.totals(c) for c in range(GROUPS)]
    for at in range(2):
        total = jnp.concatenate([part[at] for part in parts], axis=1)
        x_rows = x_ref[pl.ds(pl.multiple_of(y * block + at * piece, piece), piece), :]
        h = (x_rows.astype(F32) + total.astype(BF16).astype(F32)).astype(BF16)
        own_ref[at * piece:(at + 1) * piece, :] = h
        rows_all[0, at] = rms(h.astype(F32), g_ref[1:2, :])
    for c in range(GROUPS):
        gather.start(c)
    small.middle()
    for c in range(GROUPS):
        gather.forward(c)
    small.finish(nd_ref)
    h_dec = (tok_ref[...].astype(F32) + nd_ref[...].astype(F32)).astype(BF16)
    hd_ref[...] = h_dec.astype(F32)
    nd_ref[...] = rms(hd_ref[...], dg_ref[1:2, :])
    part_scr[...] = jnp.zeros_like(part_scr)
    reduce.drain()
    for ref in (reduce.send_a, reduce.keep_a, reduce.send_b, reduce.keep_b):
        ref[...] = jnp.zeros_like(ref)
    gather.finish()
    for copy in kv_copies:
        copy.start()
    for r in range(4):
        for half in range(2):
            i = (2 * r + half) * piece
            n_ref[i:i + piece, :] = rows_all[r, half]

    def gate_up(i, slot, n):
        tall = n.shape[0] >= 128
        gate, up = [(dot_nt(w, n) if tall else dot_nt(n, w)).astype(BF16).astype(F32) for w in (ring[3 * slot], ring[3 * slot + 1])]
        m = jax.nn.silu(gate) * up
        m = m.T if tall else m
        lane = lax.broadcasted_iota(jnp.int32, m.shape, 1)
        return jnp.where(f_at(i) + lane >= i * F_BLOCK, m, 0.0).astype(BF16)

    def down(m, slot, size, add):
        for c in range(size // N_BLOCK):
            cols = slice(c * N_BLOCK, (c + 1) * N_BLOCK)
            add(dot(m, ring[3 * slot + 2, :, cols]), cols)

    def stream_mlp(base, gu_hbm, down_hbm, size, n_rows, m_ref, add, beside):
        for copy in gu_loads(base, gu_hbm, 0):
            copy.wait()
        m_ref[0] = gate_up(0, f_slot(base), n_rows[...])

        @pl.loop(1, f_steps)
        def _(i):
            t = base + i
            f_start(t + F_SLOTS - 1)
            slot = f_slot(t)
            for copy in gu_loads(t, gu_hbm, i):
                copy.wait()
            down_load(t, down_hbm, i - 1, size).wait()
            before = m_ref[i - 1]
            after = gate_up(i, slot, n_rows[...])
            down(before, slot, size, add)
            m_ref[i] = after
            beside(i)

        t = base + f_steps
        f_start(t + F_SLOTS - 1)
        down_load(t, down_hbm, f_steps - 1, size).wait()
        down(m_ref[f_steps - 1], f_slot(t), size, add)

    def add_pre(part, cols):
        reduce.put(part, cols, True)

    stream_mlp(0, gup_hbm, dnp_hbm, group, n_ref, m_ref, add_pre, lambda i: None)
    reduce.start(0)

    @pl.loop(0, f_steps)
    def _(i):
        late_load(i).wait()
        m = m_ref[i]
        for c in range(group // N_BLOCK):
            at = c * N_BLOCK
            add_pre(dot(m, late[lax.rem(i, LATE_SLOTS), :, at:at + N_BLOCK]), slice(group + at, group + at + N_BLOCK))

        @pl.when(i + LATE_SLOTS < f_steps)
        def _():
            late_load(i + LATE_SLOTS).start()

    reduce.start(1)

    def add_dec(part, cols):
        c = cols.start // quarter
        part_scr[c, :, cols.start - c * quarter:cols.stop - c * quarter] += part

    def own_rows(c):
        cols = slice(c * group, (c + 1) * group)
        for half, total in zip((0, 1), reduce.totals(c)):
            h = own_ref[half * piece:(half + 1) * piece, cols].astype(F32)
            rows_all[0, half, :, cols] = (h + total.astype(BF16).astype(F32)).astype(BF16)
        gather.start(c)

    def between(i):
        @pl.when(i == 1)
        def _():
            reduce.middle(0)

        @pl.when(i == 5)
        def _():
            reduce.middle(1)

        @pl.when(i == 6)
        def _():
            own_rows(0)

        @pl.when(i == 8)
        def _():
            gather.forward(0)

        @pl.when(i == 9)
        def _():
            own_rows(1)

    stream_mlp(f_steps, gud_hbm, dnd_hbm, width, nd_ref, md_ref, add_dec, between)
    for r in range(4):
        small.part[r] = part_scr[lax.bitwise_xor(y, r)]
    small.start()
    gather.forward(1)
    small.middle()
    for r in range(4):
        kv_copies[r].wait_recv()
        owner = lax.bitwise_xor(y, r)
        for jj in range(heads // 4):
            k_scr[owner * (heads // 4) + jj] = kv_got[r, 0, jj]
            v_scr[owner * (heads // 4) + jj] = kv_got[r, 1, jj]
    kp_ref[...] = jnp.swapaxes(k_scr[...], 0, 1)
    vp_ref[...] = jnp.swapaxes(v_scr[...], 0, 1)
    small.finish(nd_ref)
    d_out[...] = (hd_ref[...] + nd_ref[...].astype(F32)).astype(BF16)
    reduce.drain()
    for copy in kv_copies:
        copy.wait_send()
    gather.finish()
    for r in range(4):
        owner = lax.bitwise_xor(y, r)
        for half in range(2):
            h_out[pl.ds(pl.multiple_of((2 * owner + half) * piece, piece), piece), :] = rows_all[r, half]


def finish_kernel(c_len, kt_ref, vt_ref, kc_hbm, vc_hbm, h_in, d_in, kp_in, vp_in, kn_hbm, vn_hbm, h_hbm, d_hbm, kp_hbm, vp_hbm, cache, h_buf, d_buf, kp_buf, vp_buf, in_sem, out_sem, m_in, m_out):
    batch = kt_ref.shape[0]
    moved = ((h_in, h_buf, h_hbm), (d_in, d_buf, d_hbm), (kp_in, kp_buf, kp_hbm), (vp_in, vp_buf, vp_hbm))

    def load(b, which):
        return pltpu.make_async_copy((kc_hbm, vc_hbm)[which].at[b], cache.at[which, b], in_sem.at[which, b])

    def store(b, which):
        return pltpu.make_async_copy(cache.at[which, b], (kn_hbm, vn_hbm)[which].at[b], out_sem.at[which, b])

    @pl.loop(0, batch)
    def _(b):
        load(b, 0).start()
        load(b, 1).start()

    ins = [pltpu.make_async_copy(src, mid, m_in.at[i]) for i, (src, mid, _) in enumerate(moved)]
    outs = [pltpu.make_async_copy(mid, dst, m_out.at[i]) for i, (_, mid, dst) in enumerate(moved)]
    for copy in ins:
        copy.start()

    @pl.loop(0, batch)
    def _(b):
        for which, tok in ((0, kt_ref), (1, vt_ref)):
            load(b, which).wait()
            cache[which, b, c_len[b]] = tok[b]
            store(b, which).start()

    for first, second in zip(ins, outs):
        first.wait()
        second.start()

    @pl.loop(0, batch)
    def _(b):
        store(b, 0).wait()
        store(b, 1).wait()

    for copy in outs:
        copy.wait()


def call(kernel, name, in_specs, out_specs, out_shape, scratch, us, collective_id=None):
    return pl.pallas_call(kernel, name=name, in_specs=in_specs, out_specs=out_specs, out_shape=out_shape, scratch_shapes=scratch,
                          cost_estimate=pl.CostEstimate(flops=int(us * 2e7), bytes_accessed=int(us * 3e6), transcendentals=0),
                          compiler_params=pltpu.CompilerParams(vmem_limit_bytes=62 * 2 ** 20, collective_id=collective_id, has_side_effects=collective_id is not None))


def shape(dims, dtype=F32):
    return jax.ShapeDtypeStruct(dims, dtype)


def solution(mesh):
    side = mesh.shape['side']
    inst_axes = ('pair', 'side')
    rows_spec = P(inst_axes, None)
    vec_spec = P(inst_axes)
    cache_spec = P(None, inst_axes, None, None, 'tp', None)
    prompt_spec = P(None, inst_axes, None, 'tp', None)
    in_specs = (rows_spec, vec_spec, P(None, None, None, 'tp', None), P(None, 'tp', None, None), P(None, None, 'tp', None), P(None, 'tp', None), P(None, None, None), rows_spec, cache_spec, cache_spec, vec_spec, P(None, None, None, None, 'tp', None), P(None, None, 'tp', None, None), P(None, None, 'tp', None), P(None, 'tp', None), P(None, None, None))
    out_specs = (rows_spec, rows_spec, prompt_spec, prompt_spec, cache_spec, cache_spec)

    def device_fn(prompt_x, s_len, w_qkv_pre, w_out_pre, w_gu_pre, w_down_pre, gain_pre, dec_tokens, k_cache, v_cache, c_len, w_qkv_dec, w_out_dec, w_gu_dec, w_down_dec, gain_dec):
        rows, width = prompt_x.shape
        batch = dec_tokens.shape[0]
        heads, head = w_qkv_pre.shape[3], w_qkv_pre.shape[4]
        cache_len = k_cache.shape[2]
        piece = rows // 8
        quarter = width // 4
        pairs = heads // 2
        f_steps = pl.cdiv(w_down_pre.shape[1], F_BLOCK)
        dma = pltpu.SemaphoreType.DMA
        cos_tab, sin_tab = rope_rows(max(rows, cache_len), head)
        comm = RowReduce.scratch(piece, width) + RowGather.scratch(piece, width) + ColumnSum.scratch(batch, quarter)
        flat = (batch, cache_len * heads, head)
        wide = (batch, cache_len, heads, head)
        kv_block = pltpu.VMEM((4, 2, heads // 4, rows, head), BF16)
        rows_shape, tok_shape, kv_shape, out_shape = shape((rows, width), BF16), shape((batch, heads, head), BF16), shape((rows, heads, head), BF16), shape((batch, width), BF16)
        h_out, dec_out, k_tok, v_tok, k_prompt, v_prompt = call(
            functools.partial(layer_kernel, side), 'layer', [SMEM] * 2 + [HBM] * 16, [VMEM] * 6,
            [rows_shape, out_shape, tok_shape, tok_shape, kv_shape, kv_shape],
            [pltpu.VMEM((rows, width), BF16), pltpu.VMEM((2, width), F32), pltpu.VMEM(cos_tab.shape, F32), pltpu.VMEM(cos_tab.shape, F32), pltpu.VMEM((batch, width), BF16), pltpu.VMEM((2, width), F32), dma((6,)), pltpu.VMEM((D_SLOTS, D_BLOCK, 3, heads, head), BF16), dma((D_SLOTS,)),
             pltpu.VMEM((3 * F_SLOTS, F_BLOCK, width), BF16), dma((3, F_SLOTS)), dma((2,)), pltpu.VMEM((2, ROW_SLOTS) + flat[1:], BF16), dma((2, ROW_SLOTS)),
             pltpu.VMEM((rows, width), BF16), pltpu.VMEM((3 * pairs, rows, 2 * head), F32), pltpu.VMEM((rows, heads * head), BF16), pltpu.VMEM((rows, heads * head), BF16),
             pltpu.VMEM((heads, rows, head), BF16), pltpu.VMEM((heads, rows, head), BF16),
             pltpu.VMEM((batch, width), BF16), pltpu.VMEM((batch, width), F32), pltpu.VMEM((3 * pairs, batch, 2 * head), F32), pltpu.VMEM((batch, heads, head), BF16), pltpu.VMEM((batch, heads, head), F32), pltpu.VMEM((4, batch, quarter), F32),
              pltpu.VMEM((2 * piece, width), BF16), pltpu.VMEM((f_steps, rows, F_BLOCK), BF16), pltpu.VMEM((f_steps, batch, F_BLOCK), BF16), pltpu.VMEM((LATE_SLOTS, F_BLOCK, width // GROUPS), BF16), dma((LATE_SLOTS,)), kv_block, kv_block, dma((4,)), dma((4,))] + comm, 90, 0)(
            s_len, c_len, gain_pre[0], cos_tab, sin_tab, dec_tokens, gain_dec[0], prompt_x,
            w_qkv_pre[0], w_out_pre.reshape(heads * head // F_BLOCK, F_BLOCK, width), w_qkv_dec.reshape(width, 3, heads, head),
            k_cache.reshape(flat), v_cache.reshape(flat), w_out_dec.reshape(heads * head // F_BLOCK, F_BLOCK, width),
            w_gu_pre[0], w_down_pre[0], w_gu_dec[0], w_down_dec[0])
        k_new, v_new, h_out, dec_out, k_prompt, v_prompt = call(
            finish_kernel, 'finish', [SMEM] + [VMEM] * 2 + [HBM] * 6, [HBM] * 6, [shape(wide, BF16)] * 2 + [rows_shape, out_shape, kv_shape, kv_shape],
            [pltpu.VMEM((2,) + wide, BF16), pltpu.VMEM((rows, width), BF16), pltpu.VMEM((batch, width), BF16), pltpu.VMEM((rows, heads, head), BF16), pltpu.VMEM((rows, heads, head), BF16),
             dma((2, batch)), dma((2, batch)), dma((4,)), dma((4,))], 7)(
            c_len, k_tok, v_tok, k_cache.reshape(wide), v_cache.reshape(wide), h_out, dec_out, k_prompt, v_prompt)
        prompt_shape = (1, rows, heads, 1, head)
        return h_out, dec_out, k_prompt.reshape(prompt_shape), v_prompt.reshape(prompt_shape), k_new.reshape(k_cache.shape), v_new.reshape(v_cache.shape)

    return jax.shard_map(device_fn, mesh=mesh, in_specs=in_specs, out_specs=out_specs, check_vma=False)
```
